512 devices in a mesh: groups: 2 (over y), aa: 16 (over z), ba: 16 (over x, core).
Axes of the slice: x: 8, y: 2, z: 16, core: 2. Of those that a mesh axis runs over, the one named last changes fastest.
The devices are a block of a 8x8x16 slice.
Arguments:
- alignment_state: bfloat16 [256, 512, 256], P(('groups', 'aa'), 'ba'), parts along dimension 0, may hold values from -1.5 to 1.5
- pair_state: bfloat16 [1024, 512, 128], P(('groups', 'aa'), 'ba'), parts along dimension 0, may hold values from -1.796875 to 1.796875
- alignment_mask: int32 [256, 512], P(('groups', 'aa'), 'ba'), parts along dimension 0, may hold values from 0 to 1, as said below
- left_weight: bfloat16 [256, 32], replicated, may hold values from -0.375 to 0.375
- right_weight: bfloat16 [256, 32], replicated, may hold values from -0.375 to 0.375
- outer_output_weight: bfloat16 [1024, 128], replicated, may hold values from -0.75 to 0.75
- pair_bias_weight: bfloat16 [128, 8], replicated, may hold values from -40 to 40
- query_weight: bfloat16 [256, 256], replicated, may hold values from -0.375 to 0.375
- key_weight: bfloat16 [256, 256], replicated, may hold values from -0.375 to 0.375
- value_weight: bfloat16 [256, 256], replicated, may hold values from -0.375 to 0.375
- gate_weight: bfloat16 [256, 256], replicated, may hold values from -0.375 to 0.375
- output_weight: bfloat16 [256, 256], replicated, may hold values from -1.5 to 1.5
- up_weight: bfloat16 [256, 1024], replicated, may hold values from -0.375 to 0.375
- down_weight: bfloat16 [1024, 256], replicated, may hold values from -0.1875 to 0.1875
Outputs:
- alignment_output: bfloat16 [256, 512, 256], P(('groups', 'aa'), 'ba'), parts along dimension 0
- pair_output: bfloat16 [1024, 512, 128], P(('groups', 'aa'), 'ba'), parts along dimension 0
The draws below stay inside these ranges and needn't reach their ends.
There are 2 independent parts, one for each index of `groups`. The reference program is written for one: setup_inputs(seed, part) draws one part's arguments, and reference() takes and returns one part's arrays. A program takes and returns all parts, laid end to end along the dimension named above; an argument that names none is the same for every part. Nothing has to cross between parts.
Inputs may be any that keep to these rules, and one draw needn't show every extreme that they name: `alignment_mask`: every residue of the first sequence is kept (mask 1); other entries are kept at random.
All inputs are finite; a program needn't handle non-finite values.
Results may differ from the reference program's by a relative error of at most 0.013.
The reference program's roundings to bfloat16 on the way count: a program that leaves them out, or rounds other values in their place, can miss the bound.
Values may be sent and summed in bfloat16 or wider, within the bound.
A program may use at most 128 MiB of HBM per device.

```python
import jax
import jax.numpy as jnp
from jax import lax

CHANNEL_COUNT = 256
CZ = 128
HEADS = 8
HEAD_DIM = 32
OPM_DIM = 32
TRANS = 1024
RES_DEV = 32
SEQUENCE_COUNT = 128
RESIDUE_COUNT = 512
N_BA = 16


def draw_alignment_mask(key, part):
    coins = jax.random.randint(jax.random.fold_in(key, 21), (SEQUENCE_COUNT, RESIDUE_COUNT), 0, 4)
    first_row = lax.broadcasted_iota(jnp.int32, (SEQUENCE_COUNT, RESIDUE_COUNT), 0) == 0
    return jnp.where((coins > 0) | first_row, 1, 0).astype(jnp.int32)


def draw_pair_bias_weight(key, part):
    base = jnp.clip(jax.random.normal(jax.random.fold_in(key, 11), (CZ, HEADS), jnp.float32), -4.0, 4.0)
    return (base / jnp.sqrt(jnp.float32(CZ))).astype(jnp.bfloat16)


def block_levels(own_key, shape, shards, least, high):
    def one(position, parts):
        draws = jax.random.uniform(jax.random.fold_in(jax.random.fold_in(own_key, 6), position), (parts,), jnp.float32, least / len(shards), high / len(shards))
        return jnp.repeat(jnp.exp(draws), shape[position] // parts).reshape((-1,) + (1,) * (len(shape) - position - 1))

    gain = one(*shards[0])
    for cut in shards[1:]:
        gain = gain * one(*cut)
    return gain


def scatter_about(own_key, shape, width, reach, shards=(), held_as=jnp.bfloat16):
    gain = block_levels(own_key, shape, shards, -0.22, 0.18) if shards else 1.0
    array = jax.random.normal(own_key, shape, jnp.float32) * width * gain
    return jnp.minimum(jnp.maximum(array, -reach), reach).astype(held_as)


def setup_inputs(seed: int = 0, part: int = 0) -> dict:
    keys = jax.random.split(jax.random.key(seed), 15)
    own_keys = jax.random.split(jax.random.fold_in(keys[14], part), 15)
    return {
        "alignment_state": scatter_about(own_keys[0], (SEQUENCE_COUNT, RESIDUE_COUNT, CHANNEL_COUNT), 0.25, 1.5, ((0, 16), (1, 16))),
        "pair_state": scatter_about(own_keys[1], (RESIDUE_COUNT, RESIDUE_COUNT, CZ), 0.3, 1.796875, ((0, 16), (1, 16))),
        "alignment_mask": draw_alignment_mask(jax.random.fold_in(jax.random.fold_in(keys[14], part), 71), part),
        "left_weight": scatter_about(keys[3], (CHANNEL_COUNT, OPM_DIM), CHANNEL_COUNT ** -0.5, 0.375),
        "right_weight": scatter_about(keys[4], (CHANNEL_COUNT, OPM_DIM), CHANNEL_COUNT ** -0.5, 0.375),
        "outer_output_weight": scatter_about(keys[5], (OPM_DIM * OPM_DIM, CZ), (2 * OPM_DIM) ** -0.5, 0.75),
        "pair_bias_weight": draw_pair_bias_weight(jax.random.fold_in(keys[14], 71), part),
        "query_weight": scatter_about(keys[7], (CHANNEL_COUNT, HEADS * HEAD_DIM), CHANNEL_COUNT ** -0.5, 0.375),
        "key_weight": scatter_about(keys[8], (CHANNEL_COUNT, HEADS * HEAD_DIM), CHANNEL_COUNT ** -0.5, 0.375),
        "value_weight": scatter_about(keys[9], (CHANNEL_COUNT, HEADS * HEAD_DIM), CHANNEL_COUNT ** -0.5, 0.375),
        "gate_weight": scatter_about(keys[10], (CHANNEL_COUNT, HEADS * HEAD_DIM), CHANNEL_COUNT ** -0.5, 0.375),
        "output_weight": scatter_about(keys[11], (HEADS * HEAD_DIM, CHANNEL_COUNT), (HEADS * HEAD_DIM // 16) ** -0.5, 1.5),
        "up_weight": scatter_about(keys[12], (CHANNEL_COUNT, TRANS), CHANNEL_COUNT ** -0.5, 0.375),
        "down_weight": scatter_about(keys[13], (TRANS, CHANNEL_COUNT), TRANS ** -0.5, 0.1875),
    }


def row_norm_input(values):
    center = values - lax.optimization_barrier(jnp.mean(values, axis=-1, keepdims=True))
    spread = lax.optimization_barrier(jnp.mean(center * center, axis=-1, keepdims=True))
    return center * lax.rsqrt(spread + 1e-05)

def reference(alignment_state, pair_state, alignment_mask, left_weight, right_weight, outer_output_weight, pair_bias_weight, query_weight, key_weight, value_weight, gate_weight, output_weight, up_weight, down_weight):
    layer_normed = row_norm_input(alignment_state.astype(jnp.float32)).astype(jnp.bfloat16)
    flat_rows = layer_normed.reshape(SEQUENCE_COUNT * RESIDUE_COUNT, CHANNEL_COUNT)
    row_keep_mask = alignment_mask.astype(jnp.float32)
    left_fac = (jnp.dot(flat_rows, left_weight, preferred_element_type=jnp.float32).reshape(SEQUENCE_COUNT, RESIDUE_COUNT, OPM_DIM) * row_keep_mask[:, :, None]).astype(jnp.bfloat16)
    right_fac = (jnp.dot(flat_rows, right_weight, preferred_element_type=jnp.float32).reshape(SEQUENCE_COUNT, RESIDUE_COUNT, OPM_DIM) * row_keep_mask[:, :, None]).astype(jnp.bfloat16)
    pair_count = jnp.dot(row_keep_mask.T, row_keep_mask, precision=lax.Precision.HIGHEST)
    left_flat = left_fac.reshape(SEQUENCE_COUNT, RESIDUE_COUNT * OPM_DIM)
    right_flat = right_fac.reshape(SEQUENCE_COUNT, RESIDUE_COUNT * OPM_DIM)

    def outer_block(block_index):
        left_part = lax.dynamic_slice_in_dim(left_flat, block_index * (RES_DEV * OPM_DIM), RES_DEV * OPM_DIM, 1)
        outer_sum = lax.dot_general(left_part, right_flat, (((0,), (0,)), ((), ())), preferred_element_type=jnp.float32)
        outer_sum = outer_sum.reshape(RES_DEV, OPM_DIM, RESIDUE_COUNT, OPM_DIM).transpose(0, 2, 1, 3)
        outer_sum = outer_sum.reshape(RES_DEV * RESIDUE_COUNT, OPM_DIM * OPM_DIM).astype(jnp.bfloat16)
        return jnp.dot(outer_sum, outer_output_weight, preferred_element_type=jnp.float32).reshape(RES_DEV, RESIDUE_COUNT, CZ)
    update = lax.map(outer_block, jnp.arange(N_BA, dtype=jnp.int32)).reshape(RESIDUE_COUNT, RESIDUE_COUNT, CZ)
    pair_output = (pair_state.astype(jnp.float32) + update / pair_count[:, :, None]).astype(jnp.bfloat16)
    pair_normed = row_norm_input(pair_output.astype(jnp.float32)).astype(jnp.bfloat16)
    bias_full = jnp.dot(pair_normed.reshape(RESIDUE_COUNT * RESIDUE_COUNT, CZ), pair_bias_weight, preferred_element_type=jnp.float32)
    bias_full = bias_full.reshape(RESIDUE_COUNT, RESIDUE_COUNT, HEADS).transpose(2, 0, 1)
    score_scale = HEAD_DIM ** (-0.5)
    query_all = (jnp.dot(flat_rows, query_weight, preferred_element_type=jnp.float32) * score_scale).astype(jnp.bfloat16).reshape(SEQUENCE_COUNT, RESIDUE_COUNT, HEADS, HEAD_DIM)
    key_all = jnp.dot(flat_rows, key_weight, preferred_element_type=jnp.float32).astype(jnp.bfloat16).reshape(SEQUENCE_COUNT, RESIDUE_COUNT, HEADS, HEAD_DIM)
    value_all = jnp.dot(flat_rows, value_weight, preferred_element_type=jnp.float32).astype(jnp.bfloat16).reshape(SEQUENCE_COUNT, RESIDUE_COUNT, HEADS, HEAD_DIM)
    gate_act = jax.nn.sigmoid(jnp.dot(flat_rows, gate_weight, preferred_element_type=jnp.float32))

    def per_sequence(members):
        query_one, key_one, value_one, valid_one = members
        scores = jnp.einsum('ihd,jhd->hij', query_one.astype(jnp.float32), key_one.astype(jnp.float32), precision=lax.Precision.HIGHEST) + bias_full
        scores = jnp.where(valid_one[None, None, :] > 0, scores, -1000000000.0)
        weights_raw = jnp.exp(scores - lax.optimization_barrier(jnp.max(scores, axis=-1, keepdims=True)))
        mass_total = lax.optimization_barrier(jnp.sum(weights_raw, axis=-1))
        probs_half = lax.optimization_barrier(weights_raw.astype(jnp.bfloat16)).astype(jnp.float32)
        mixed_vals = jnp.einsum('hij,jhd->ihd', probs_half, value_one.astype(jnp.float32), precision=lax.Precision.HIGHEST)
        return mixed_vals / jnp.transpose(mass_total)[:, :, None]
    attended = lax.map(per_sequence, (query_all, key_all, value_all, row_keep_mask)).reshape(SEQUENCE_COUNT * RESIDUE_COUNT, HEADS * HEAD_DIM)
    gated_row_output = (attended * gate_act).astype(jnp.bfloat16)
    alignment_middle = alignment_state.astype(jnp.float32) + jnp.dot(gated_row_output, output_weight, preferred_element_type=jnp.float32).reshape(SEQUENCE_COUNT, RESIDUE_COUNT, CHANNEL_COUNT)
    middle_normed = row_norm_input(alignment_middle).astype(jnp.bfloat16).reshape(SEQUENCE_COUNT * RESIDUE_COUNT, CHANNEL_COUNT)
    hidden_units = jax.nn.relu(jnp.dot(middle_normed, up_weight, preferred_element_type=jnp.float32)).astype(jnp.bfloat16)
    alignment_output = (alignment_middle + jnp.dot(hidden_units, down_weight, preferred_element_type=jnp.float32).reshape(SEQUENCE_COUNT, RESIDUE_COUNT, CHANNEL_COUNT)).astype(jnp.bfloat16)
    return (alignment_output, pair_output)
```

```python
import functools

import jax
import jax.numpy as jnp
from jax import lax
from jax.experimental import pallas as pl
from jax.experimental.pallas import tpu as pltpu
from jax.sharding import PartitionSpec as P

F32 = jnp.float32
BF16 = jnp.bfloat16
NT = (((1,), (1,)), ((), ()))


def mm(x, y):
    return jnp.dot(x, y, preferred_element_type=F32)


def mm_nt(x, y):
    return lax.dot_general(x, y, NT, preferred_element_type=F32)


def row_norm(values):
    center = values - jnp.mean(values, axis=-1, keepdims=True)
    spread = jnp.mean(center * center, axis=-1, keepdims=True)
    return center * lax.rsqrt(spread + 1e-05)


def near_to_far(t):
    return ((t + 1) // 2) * (2 * (t % 2) - 1)


def body(
    n,
    state_ref,
    pair_ref,
    mask_ref,
    left_ref,
    right_ref,
    outer_ref,
    pbw_ref,
    wq_ref,
    wk_ref,
    wv_ref,
    wg_ref,
    wo_ref,
    up_ref,
    down_ref,
    msa_out,
    pair_out,
    rows,
    nf,
    lx,
    lz,
    rz,
    tz,
    bx,
    lf,
    rf,
    rt,
    rt2,
    lb,
    wf,
    bd,
    lhs,
    upd,
    pn,
    bi,
    bh,
    kv,
    sc,
    qs,
    gs,
    vm,
    gated,
    lx_s,
    lx_r,
    lz_s,
    lz_r,
    rz_s,
    rz_r,
    x1_s,
    x1_r,
    xf_s,
    xf_r,
    tz_s,
    tz_r,
    bx_s,
    bx_r,
):
    a = lax.axis_index("aa")
    b = lax.axis_index("ba")
    core = b % 2
    chip = b // 2
    chips = n // 2
    partner = chip * 2 + 1 - core
    ns = state_ref.shape[0]
    res = state_ref.shape[1]
    ch = state_ref.shape[2]
    half = ns // 2
    opm = left_ref.shape[1]
    cz = pair_ref.shape[2]
    heads = pbw_ref.shape[1]
    wide = res * opm
    per = 128 // opm

    def row_peer(t):
        c = (chip + near_to_far(t // 2) + chips) % chips
        return c * 2 + t % 2

    def col_peer(t):
        return (a + near_to_far(t) + n) % n

    barrier = pltpu.get_barrier_semaphore()

    def greet(t, _):
        pl.semaphore_signal(
            barrier, inc=1, device_id={"ba": (b + t) % n}, device_id_type=pl.DeviceIdType.MESH
        )
        pl.semaphore_signal(
            barrier, inc=1, device_id={"aa": (a + t) % n}, device_id_type=pl.DeviceIdType.MESH
        )
        return 0

    lax.fori_loop(1, n, greet, 0)

    state = state_ref[...].reshape(ns * res, ch).astype(F32)
    normed = row_norm(state).astype(BF16)
    rows[:, b] = normed.reshape(ns, res, ch)
    for q in range(ch // 128):
        nf[q] = normed[:, q * 128 : (q + 1) * 128].astype(F32)
    by_res = jnp.concatenate(
        [
            jnp.concatenate(
                [nf[q, pl.ds(r, ns, stride=res), :] for r in range(res)], axis=0
            ).astype(BF16)
            for q in range(ch // 128)
        ],
        axis=1,
    )
    lane = lax.broadcasted_iota(jnp.int32, (opm, 128), 1)
    line = lax.broadcasted_iota(jnp.int32, (opm, 128), 0)
    rep = jnp.where(lane % opm == line, 1.0, 0.0).astype(BF16)
    seg = lax.broadcasted_iota(jnp.int32, (ns, 128), 1) // opm
    keep = mask_ref[...].astype(F32).astype(BF16)
    lane_w = lax.broadcasted_iota(jnp.int32, (res, wide), 1) // opm
    line_w = lax.broadcasted_iota(jnp.int32, (res, wide), 0)
    keep_wide = mm(keep, jnp.where(lane_w == line_w, 1.0, 0.0).astype(BF16))
    keep_rep = mm(keep, rep).astype(BF16)

    def pick(parts):
        out = parts[0]
        for k in range(1, per):
            out = jnp.where(seg == k, parts[k], out)
        return out

    def factor(w_ref):
        w4 = mm(w_ref[...], rep).astype(BF16)
        y = mm(by_res, w4)
        cols = [
            pick([y[(q * per + k) * ns : (q * per + k + 1) * ns] for k in range(per)])
            for q in range(res // per)
        ]
        return (jnp.concatenate(cols, axis=1) * keep_wide).astype(BF16)

    lx[b, :, :wide] = factor(left_ref)
    lx[b, :, wide:] = keep_rep
    rz[a, :, :wide] = factor(right_ref)
    rz[a, :, wide:] = keep_rep

    pl.semaphore_wait(barrier, 2 * (n - 1))

    def to_row(buf, src, i, who, ss, rs):
        return pltpu.make_async_remote_copy(
            src_ref=src,
            dst_ref=buf,
            send_sem=ss.at[who],
            recv_sem=rs.at[i],
            device_id={"ba": who},
            device_id_type=pl.DeviceIdType.MESH,
        )

    def to_col(buf, src, i, who, ss, rs):
        return pltpu.make_async_remote_copy(
            src_ref=src,
            dst_ref=buf,
            send_sem=ss.at[who],
            recv_sem=rs.at[i],
            device_id={"aa": who},
            device_id_type=pl.DeviceIdType.MESH,
        )

    def lx_copy(i, who):
        return to_row(lx.at[i], lx.at[i], i, who, lx_s, lx_r)

    def rz_copy(i, who):
        return to_col(rz.at[i], rz.at[i], i, who, rz_s, rz_r)

    def lz_copy(i, who):
        return to_col(lz.at[i], lx.at[who], i, who, lz_s, lz_r)

    def tz_copy(i, who):
        return to_col(tz.at[i], tz.at[i], i, who, tz_s, tz_r)

    def bx_copy(i, who):
        return to_row(bx.at[i], tz.at[who], i, who, bx_s, bx_r)

    def x1_copy(i, who, c):
        part = rows.at[pl.ds(half * c, half), i]
        return to_row(part, part, i, who, x1_s, x1_r)

    def xf_copy(i):
        part = rows.at[pl.ds(half * core, half), i]
        return pltpu.make_async_remote_copy(
            src_ref=part,
            dst_ref=part,
            send_sem=xf_s.at[i],
            recv_sem=xf_r.at[i],
            device_id={"ba": partner},
            device_id_type=pl.DeviceIdType.MESH,
        )

    def in_part(i):
        part = rows.at[pl.ds(half * (1 - core), half), i]
        return pltpu.make_async_remote_copy(
            src_ref=part,
            dst_ref=part,
            send_sem=xf_s.at[i],
            recv_sem=xf_r.at[i],
            device_id={"ba": partner},
            device_id_type=pl.DeviceIdType.MESH,
        )

    def start_lr(t, _):
        far = n - 1 - t
        lx_copy(b, row_peer(far)).start()
        rz_copy(a, col_peer(far)).start()
        return 0

    def start_l_off(t, _):
        lx_copy(b, row_peer(n - 1 - t)).start()
        return 0

    def start_r(t, _):
        rz_copy(a, col_peer(n - 1 - t)).start()
        return 0

    lx_copy(b, partner).start()
    lax.fori_loop(0, n - 2, start_l_off, 0)
    lax.fori_loop(0, n - 1, start_r, 0)

    def start_x(t, _):
        who = row_peer(n - 1 - t)
        x1_copy(b, who, who % 2).start()
        return 0

    lax.fori_loop(0, n - 2, start_x, 0)
    x1_copy(b, partner, 1 - core).start()
    xf_copy(b).start()

    wf[...] = outer_ref[...].astype(F32)

    def build(d, _):
        w = wf[pl.ds(d, opm, stride=opm), :].astype(BF16)
        zero = jnp.zeros_like(w)
        for k in range(per):
            bd[pl.ds(d * 128 + k * opm, opm), :] = jnp.concatenate(
                [w if m == k else zero for m in range(per)], axis=1
            )
        return 0

    lax.fori_loop(0, opm, build, 0)

    def pass_left(t, _):
        i = row_peer(t)

        @pl.when(i != b)
        def _():
            lx_copy(i, b).wait_recv()

        @pl.when(i != a)
        def _():
            lz_copy(a, i).start()

        @pl.when(i == a)
        def _():
            lz[a] = lx[i]

        return 0

    lax.fori_loop(0, n, pass_left, 0)

    qs[...] = (mm(normed, wq_ref[...]) * ((ch // heads) ** (-0.5))).astype(BF16)
    gs[...] = jax.nn.sigmoid(mm(normed, wg_ref[...]))
    for q in range(n // per):
        vm[:, q * 128 : (q + 1) * 128] = pick(
            [lx[q * per + k, :, wide:].astype(F32) for k in range(per)]
        )

    def land_right(t, _):
        i = col_peer(t)

        @pl.when(i != a)
        def _():
            rz_copy(i, a).wait_recv()

        rf[pl.ds(pl.multiple_of(i * ns, ns), ns), :] = rz[i].astype(F32)
        return 0

    lax.fori_loop(0, n, land_right, 0)
    for q in range(wide // 128):
        rt[q * 128 : (q + 1) * 128, :] = rf[:, q * 128 : (q + 1) * 128].T

    def reorder(d, _):
        rt2[pl.ds(pl.multiple_of(d * res, res), res), :] = rt[
            pl.ds(d, res, stride=opm), :
        ].astype(BF16)
        return 0

    lax.fori_loop(0, opm, reorder, 0)

    def land_left(t, _):
        i = col_peer(t)

        @pl.when(i != a)
        def _():
            lz_copy(i, a).wait_recv()

        lf[pl.ds(pl.multiple_of(i * ns, ns), ns), :] = lz[i].astype(F32)
        return 0

    lax.fori_loop(0, n, land_left, 0)

    groups = res // per
    for g in range(groups):
        lb[g] = lf[:, g * 128 : (g + 1) * 128].astype(BF16)

    def outer(g, _):
        block = mm(rt2[...], lb[g]).astype(BF16)
        for d in range(opm):
            lhs[pl.ds(pl.multiple_of(g * res, res), res), d * 128 : (d + 1) * 128] = block[
                d * res : (d + 1) * res
            ]
        return 0

    lax.fori_loop(0, groups, outer, 0)
    upd[...] = mm(lhs[...], bd[...])
    count = mm(rf[:, wide:].T.astype(BF16), lf[:, wide:].astype(BF16))
    inverse = 1.0 / count[:res]
    for i in range(res):
        block = upd[(i // per) * res : (i // per + 1) * res, (i % per) * 128 : (i % per + 1) * 128]
        fresh = (pair_ref[i].astype(F32) + block * inverse[:, i : i + 1]).astype(BF16)
        pair_out[i] = fresh
        pn[i * res : (i + 1) * res, :] = row_norm(fresh.astype(F32)).astype(BF16)
    eye_l = lax.broadcasted_iota(jnp.int32, (heads, heads), 1)
    eye_s = lax.broadcasted_iota(jnp.int32, (heads, heads), 0)
    eye = jnp.where(eye_l == eye_s, 1.0, 0.0).astype(BF16)
    pbw_t = mm_nt(eye, pbw_ref[...]).astype(BF16)
    tz[a] = mm_nt(pbw_t, pn[...])

    def start_bias(t, _):
        tz_copy(a, col_peer(n - 1 - t)).start()
        return 0

    lax.fori_loop(0, n - 1, start_bias, 0)

    def pass_rows(t, _):
        i = row_peer(t)
        x1_copy(i, b, core).wait_recv()
        xf_copy(i).start()
        return 0

    x1_copy(partner, b, core).wait_recv()
    lax.fori_loop(2, n, pass_rows, 0)
    in_part(partner).wait_recv()

    def land_rows(t, _):
        in_part(row_peer(t)).wait_recv()
        return 0

    lax.fori_loop(2, n, land_rows, 0)

    head_lane = lax.broadcasted_iota(jnp.int32, (res, ch), 1) // (ch // heads)

    def score(s, _):
        x = rows[s].reshape(n * res, ch)
        key = mm(x, wk_ref[...]).astype(BF16)
        kv[s] = mm(x, wv_ref[...]).astype(BF16)
        q = qs[pl.ds(pl.multiple_of(s * res, res), res), :].astype(F32)
        query = jnp.concatenate(
            [jnp.where(head_lane == h, q, 0.0) for h in range(heads)], axis=0
        ).astype(BF16)
        sc[s] = mm_nt(query, key)
        return 0

    lax.fori_loop(0, ns, score, 0)

    def pass_bias(t, _):
        i = col_peer(t)

        @pl.when(i != a)
        def _():
            tz_copy(i, a).wait_recv()

        @pl.when(i != b)
        def _():
            bx_copy(b, i).start()

        @pl.when(i == b)
        def _():
            bx[b] = tz[i]

        return 0

    lax.fori_loop(0, n, pass_bias, 0)

    def land_bias(t, _):
        i = (b + t) % n
        bx_copy(i, b).wait_recv()
        return 0

    lax.fori_loop(1, n, land_bias, 0)

    for v in range(res // per):
        for q in range(n // per):
            cut = [bx[q * per + k, :, v * 128 : (v + 1) * 128] for k in range(per)]
            turned = [cut[0]] + [pltpu.roll(cut[k], opm * k, 1) for k in range(1, per)]
            for m in range(per):
                mixed = pick([turned[(k - m) % per] for k in range(per)])
                if m:
                    mixed = pltpu.roll(mixed, 128 - opm * m, 1)
                i = v * per + m
                bi[q, i * heads : (i + 1) * heads, :] = mixed
    for h in range(heads):
        for q in range(n // per):
            bh[h * res : (h + 1) * res, q * 128 : (q + 1) * 128] = bi[
                q, pl.ds(h, res, stride=heads), :
            ]

    def attend(s, _):
        valid = vm[pl.ds(s, 1), :]
        scores = jnp.where(valid > 0, sc[s] + bh[...], -1000000000.0)
        top = jnp.max(scores, axis=-1, keepdims=True)
        raw = jnp.exp(scores - top)
        mass = jnp.sum(raw, axis=-1, keepdims=True)
        mixed = mm(raw.astype(BF16), kv[s]) / mass
        out = mixed[:res]
        for h in range(1, heads):
            out = jnp.where(head_lane == h, mixed[h * res : (h + 1) * res], out)
        at = pl.ds(pl.multiple_of(s * res, res), res)
        gated[at, :] = (out * gs[at, :]).astype(BF16)
        return 0

    lax.fori_loop(0, ns, attend, 0)

    middle = state + mm(gated[...], wo_ref[...])
    hidden = jnp.maximum(mm(row_norm(middle).astype(BF16), up_ref[...]), 0.0).astype(BF16)
    final = middle + mm(hidden, down_ref[...])
    msa_out[...] = final.astype(BF16).reshape(ns, res, ch)

    def drain(t, _):
        who = (b + t) % n
        lx_copy(b, who).wait_send()
        bx_copy(b, who).wait_send()
        up_to = (a + t) % n
        rz_copy(a, up_to).wait_send()
        lz_copy(a, up_to).wait_send()
        tz_copy(a, up_to).wait_send()
        x1_copy(b, who, who % 2).wait_send()
        return 0

    lax.fori_loop(1, n, drain, 0)

    def drain_rows(t, _):
        xf_copy(row_peer(t)).wait_send()
        return 0

    lax.fori_loop(2, n, drain_rows, 0)
    xf_copy(b).wait_send()


def per_device(n, *args):
    state, pair, mask, left, _, _, pbw = args[:7]
    ns, res, ch = state.shape
    opm, heads, cz = left.shape[1], pbw.shape[1], pair.shape[2]
    wide = res * opm
    per = 128 // opm
    groups = res // per
    keys = n * res
    dma = pltpu.SemaphoreType.DMA((n,))
    vmem = pl.BlockSpec(memory_space=pltpu.VMEM)
    return tuple(
        pl.pallas_call(
            functools.partial(body, n),
            out_shape=(
                jax.ShapeDtypeStruct(state.shape, BF16),
                jax.ShapeDtypeStruct(pair.shape, BF16),
            ),
            in_specs=[vmem] * len(args),
            out_specs=(vmem, vmem),
            scratch_shapes=[
                pltpu.VMEM((ns, n, res, ch), BF16),
                pltpu.VMEM((ch // 128, ns * res, 128), F32),
                pltpu.VMEM((n, ns, wide + 128), BF16),
                pltpu.VMEM((n, ns, wide + 128), BF16),
                pltpu.VMEM((n, ns, wide + 128), BF16),
                pltpu.VMEM((n, heads, res * res), F32),
                pltpu.VMEM((n, heads, res * res), F32),
                pltpu.VMEM((n * ns, wide + 128), F32),
                pltpu.VMEM((n * ns, wide + 128), F32),
                pltpu.VMEM((wide, n * ns), F32),
                pltpu.VMEM((wide, n * ns), BF16),
                pltpu.VMEM((groups, n * ns, 128), BF16),
                pltpu.VMEM((opm * opm, cz), F32),
                pltpu.VMEM((opm * 128, per * cz), BF16),
                pltpu.VMEM((groups * res, opm * 128), BF16),
                pltpu.VMEM((groups * res, per * cz), F32),
                pltpu.VMEM((res * res, cz), BF16),
                pltpu.VMEM((keys // 128, res * heads, 128), F32),
                pltpu.VMEM((heads * res, keys), F32),
                pltpu.VMEM((ns, keys, ch), BF16),
                pltpu.VMEM((ns, heads * res, keys), F32),
                pltpu.VMEM((ns * res, ch), BF16),
                pltpu.VMEM((ns * res, ch), F32),
                pltpu.VMEM((ns, keys), F32),
                pltpu.VMEM((ns * res, ch), BF16),
            ]
            + [dma] * 14,
            compiler_params=pltpu.CompilerParams(collective_id=0, has_side_effects=True),
        )(*args)
    )


def solution(mesh):
    spec = P(("groups", "aa"), "ba", None)
    return jax.shard_map(
        functools.partial(per_device, mesh.shape["ba"]),
        mesh=mesh,
        in_specs=(spec, spec, P(("groups", "aa"), "ba")) + (P(),) * 11,
        out_specs=(spec, spec),
        check_vma=False,
    )
```

```python
import functools

import jax
import jax.numpy as jnp
from jax import lax
from jax.experimental import pallas as pl
from jax.experimental.pallas import tpu as pltpu
from jax.sharding import PartitionSpec as P

F32 = jnp.float32
BF16 = jnp.bfloat16
NT = (((1,), (1,)), ((), ()))


def mm(x, y):
    return jnp.dot(x, y, preferred_element_type=F32)


def mm_nt(x, y):
    return lax.dot_general(x, y, NT, preferred_element_type=F32)


def row_norm(values):
    center = values - jnp.mean(values, axis=-1, keepdims=True)
    spread = jnp.mean(center * center, axis=-1, keepdims=True)
    return center * lax.rsqrt(spread + 1e-05)


def near_to_far(t):
    return ((t + 1) // 2) * (2 * (t % 2) - 1)


def body(
    n,
    state_ref,
    pair_hbm,
    mask_ref,
    left_ref,
    right_ref,
    outer_hbm,
    pbw_ref,
    wq_hbm,
    wk_hbm,
    wv_hbm,
    wg_hbm,
    wo_hbm,
    up_hbm,
    down_hbm,
    msa_hbm_out,
    pair_hbm_out,
    pair_ref,
    outer_ref,
    wq_ref,
    wk_ref,
    wv_ref,
    wg_ref,
    wo_ref,
    up_ref,
    down_ref,
    pair_out,
    msa_out,
    load_sem,
    store_sem,
    rows,
    nf,
    ls,
    lx,
    lz,
    rz,
    tz,
    bx,
    lf,
    rf,
    rt,
    rt2,
    lb,
    wf,
    bd,
    lhs,
    upd,
    pn,
    bi,
    bh,
    kv,
    sc,
    qs,
    gs,
    vm,
    gated,
    lx_s,
    lx_r,
    lz_s,
    lz_r,
    lf_s,
    lf_r,
    rz_s,
    rz_r,
    x1_s,
    x1_r,
    xr_s,
    xf_s,
    xf_r,
    tz_s,
    tz_r,
    bx_s,
    bx_r,
):
    a = lax.axis_index("aa")
    b = lax.axis_index("ba")
    core = b % 2
    chip = b // 2
    chips = n // 2
    partner = chip * 2 + 1 - core
    ns = state_ref.shape[0]
    res = state_ref.shape[1]
    ch = state_ref.shape[2]
    half = ns // 2
    opm = left_ref.shape[0]
    cz = pair_ref.shape[2]
    heads = pbw_ref.shape[0]
    wide = res * opm
    per = 128 // opm
    span = wide // 2

    hbm = (outer_hbm, wq_hbm, wg_hbm, pair_hbm, wk_hbm, wv_hbm, wo_hbm, up_hbm, down_hbm)
    local = (outer_ref, wq_ref, wg_ref, pair_ref, wk_ref, wv_ref, wo_ref, up_ref, down_ref)
    loads = [
        pltpu.make_async_copy(src, dst, load_sem.at[k])
        for k, (src, dst) in enumerate(zip(hbm, local))
    ]

    def row_peer(t):
        c = (chip + near_to_far(t // 2) + chips) % chips
        return c * 2 + t % 2

    def col_peer(t):
        return (a + near_to_far(t) + n) % n

    barrier = pltpu.get_barrier_semaphore()

    def greet(t, _):
        pl.semaphore_signal(
            barrier, inc=1, device_id={"ba": (b + t) % n}, device_id_type=pl.DeviceIdType.MESH
        )
        pl.semaphore_signal(
            barrier, inc=1, device_id={"aa": (a + t) % n}, device_id_type=pl.DeviceIdType.MESH
        )
        return 0

    lax.fori_loop(1, n, greet, 0)

    for load in loads:
        load.start()

    state = state_ref[...].reshape(ns * res, ch).astype(F32)
    normed = row_norm(state).astype(BF16)
    rows[:, b] = normed.reshape(ns, res, ch)
    for q in range(ch // 128):
        nf[q] = normed[:, q * 128 : (q + 1) * 128].astype(F32)
    by_res = jnp.concatenate(
        [
            jnp.concatenate(
                [nf[q, pl.ds(r, ns, stride=res), :] for r in range(res)], axis=0
            ).astype(BF16)
            for q in range(ch // 128)
        ],
        axis=1,
    )
    lane = lax.broadcasted_iota(jnp.int32, (opm, 128), 1)
    line = lax.broadcasted_iota(jnp.int32, (opm, 128), 0)
    rep = jnp.where(lane % opm == line, 1.0, 0.0).astype(BF16)
    lane_t = lax.broadcasted_iota(jnp.int32, (128, opm), 1)
    line_t = lax.broadcasted_iota(jnp.int32, (128, opm), 0)
    rep_t = jnp.where(line_t % opm == lane_t, 1.0, 0.0).astype(BF16)
    seg = lax.broadcasted_iota(jnp.int32, (ns, 128), 1) // opm
    keep = mask_ref[...].astype(F32).astype(BF16)
    lane_w = lax.broadcasted_iota(jnp.int32, (res, wide), 1) // opm
    line_w = lax.broadcasted_iota(jnp.int32, (res, wide), 0)
    keep_wide = mm(keep, jnp.where(lane_w == line_w, 1.0, 0.0).astype(BF16))
    keep_rep = mm(keep, rep).astype(BF16)

    def pick(parts):
        out = parts[0]
        for k in range(1, per):
            out = jnp.where(seg == k, parts[k], out)
        return out

    def factor(w_ref):
        y = mm_nt(by_res, mm(rep_t, w_ref[...]).astype(BF16))
        cols = [
            pick([y[(q * per + k) * ns : (q * per + k + 1) * ns] for k in range(per)])
            for q in range(res // per)
        ]
        return (jnp.concatenate(cols, axis=1) * keep_wide).astype(BF16)

    left = factor(left_ref)
    for k in range(2):
        ls[k, :, :span] = left[:, k * span : (k + 1) * span]
        ls[k, :, span:] = keep_rep
    lx[b] = ls[core]
    rz[a, :, :wide] = factor(right_ref)
    rz[a, :, wide:] = keep_rep

    pl.semaphore_wait(barrier, 2 * (n - 1))

    def to_row(buf, src, i, who, ss, rs):
        return pltpu.make_async_remote_copy(
            src_ref=src,
            dst_ref=buf,
            send_sem=ss.at[who],
            recv_sem=rs.at[i],
            device_id={"ba": who},
            device_id_type=pl.DeviceIdType.MESH,
        )

    def to_col(buf, src, i, who, ss, rs):
        return pltpu.make_async_remote_copy(
            src_ref=src,
            dst_ref=buf,
            send_sem=ss.at[who],
            recv_sem=rs.at[i],
            device_id={"aa": who},
            device_id_type=pl.DeviceIdType.MESH,
        )

    def lx_copy(i, who):
        return to_row(lx.at[i], ls.at[who % 2], i, who, lx_s, lx_r)

    def lz_copy(i, who):
        return to_col(lz.at[i, core], lx.at[who], i, who, lz_s, lz_r)

    def lf_copy(i, k, src=None):
        part = lz.at[i, k]
        return pltpu.make_async_remote_copy(
            src_ref=part if src is None else src,
            dst_ref=part,
            send_sem=lf_s.at[i],
            recv_sem=lf_r.at[i],
            device_id={"ba": partner},
            device_id_type=pl.DeviceIdType.MESH,
        )

    def bx_copy(i, who):
        return to_row(bx.at[i], tz.at[who], i, who, bx_s, bx_r)

    turn = n // 2

    def hop(buf, ss, rs, d, step, way):
        i = (a + n - way * d) % n
        part = buf.at[i]
        return pltpu.make_async_remote_copy(
            src_ref=part,
            dst_ref=part,
            send_sem=ss.at[d + step - 1 if way > 0 else turn + d + step - 1],
            recv_sem=rs.at[i],
            device_id={"aa": (a + n + way * step) % n},
            device_id_type=pl.DeviceIdType.MESH,
        )

    def spread(buf, ss, rs, d, reach, wait=False):
        def one(step, way):
            copy = hop(buf, ss, rs, d, step, way)
            if wait:
                copy.wait_send()
            else:
                copy.start()

        for step in range(min(reach, turn - d), 0, -1):
            for way in (1, -1):
                if d + step < turn:
                    one(step, way)
                else:
                    pl.when(core == (1 - way) // 2)(functools.partial(one, step, way))

    def ring(buf, ss, rs, reach, first, last, landed):
        for d in range(first, last + 1):
            for way in (1, -1):
                if d < turn or way > 0:
                    hop(buf, ss, rs, d, 0, way).wait_recv()
            if d % reach == 0:
                spread(buf, ss, rs, d, reach)
            for way in (1, -1):
                if d < turn or way > 0:
                    landed((a + n - way * d) % n)

    def ring_sent(buf, ss, rs, reach):
        for d in range(0, turn, reach):
            spread(buf, ss, rs, d, reach, wait=True)

    across = chips // 2

    def x_to(i, c, step, way, sem):
        part = rows.at[pl.ds(half * c, half), i]
        who = ((chip + chips + way * step) % chips) * 2 + c
        return pltpu.make_async_remote_copy(
            src_ref=part,
            dst_ref=part,
            send_sem=sem,
            recv_sem=x1_r.at[i],
            device_id={"ba": who},
            device_id_type=pl.DeviceIdType.MESH,
        )

    def x_first(wait=False):
        def one(step, way, c):
            k = (2 * step - 2 + (1 - way) // 2) * 2 + c
            copy = x_to(b, c, step, way, x1_s.at[k])
            if wait:
                copy.wait_send()
            else:
                copy.start()

        for step in range(min(2, across), 0, -1):
            for way in (1, -1):
                for c in range(2):
                    if step < across:
                        one(step, way, c)
                    else:
                        pl.when(core == (1 - way) // 2)(functools.partial(one, step, way, c))

    def x_on(wait=False):
        for step in range(min(2, across - 2), 0, -1):
            for way in (1, -1):
                for c in range(2):
                    if 2 + step < across or c == (1 - way) // 2:
                        i = ((chip + chips - 2 * way) % chips) * 2 + c
                        k = (2 * step - 2 + (1 - way) // 2) * 2 + c
                        copy = x_to(i, core, step, way, xr_s.at[k])
                        if wait:
                            copy.wait_send()
                        else:
                            copy.start()

    def x_blocks(first, last):
        return [
            ((chip + chips - way * d) % chips) * 2 + c
            for d in range(first, min(last, across) + 1)
            for way in (1, -1)
            if d < across or way > 0
            for c in range(2)
        ]

    def x1_copy(i, who, c):
        part = rows.at[pl.ds(half * c, half), i]
        return to_row(part, part, i, who, x1_s, x1_r)

    def xf_copy(i):
        part = rows.at[pl.ds(half * core, half), i]
        return pltpu.make_async_remote_copy(
            src_ref=part,
            dst_ref=part,
            send_sem=xf_s.at[i],
            recv_sem=xf_r.at[i],
            device_id={"ba": partner},
            device_id_type=pl.DeviceIdType.MESH,
        )

    def in_part(i):
        part = rows.at[pl.ds(half * (1 - core), half), i]
        return pltpu.make_async_remote_copy(
            src_ref=part,
            dst_ref=part,
            send_sem=xf_s.at[i],
            recv_sem=xf_r.at[i],
            device_id={"ba": partner},
            device_id_type=pl.DeviceIdType.MESH,
        )

    def start_l_off(t, _):
        lx_copy(b, row_peer(n - 1 - t)).start()
        return 0

    lx_copy(b, partner).start()
    lax.fori_loop(0, n - 2, start_l_off, 0)
    spread(rz, rz_s, rz_r, 0, 4)

    loads[0].wait()
    wf[...] = outer_ref[...].astype(F32)

    def build(d, _):
        w = wf[pl.ds(d, opm, stride=opm), :].astype(BF16)
        zero = jnp.zeros_like(w)
        for k in range(per):
            bd[pl.ds(d * 128 + k * opm, opm), :] = jnp.concatenate(
                [w if m == k else zero for m in range(per)], axis=1
            )
        return 0

    lax.fori_loop(0, opm, build, 0)

    def pass_left(t, _):
        i = row_peer(t)

        @pl.when(i != b)
        def _():
            lx_copy(i, b).wait_recv()

        @pl.when(i != a)
        def _():
            lz_copy(a, i).start()

        @pl.when(i == a)
        def _():
            lz[a, core] = lx[i]
            lf_copy(a, core, lx.at[i]).start()

        return 0

    def land_right(i):
        rf[pl.ds(pl.multiple_of(i * ns, ns), ns), :] = rz[i].astype(F32)

    lax.fori_loop(0, n * 5 // 8, pass_left, 0)
    land_right(a)
    ring(rz, rz_s, rz_r, 4, 1, min(4, turn), land_right)
    x_first()
    x1_copy(b, partner, 1 - core).start()
    xf_copy(b).start()
    lax.fori_loop(n * 5 // 8, n, pass_left, 0)

    loads[1].wait()
    loads[2].wait()
    qs[...] = (mm(normed, wq_ref[...]) * ((ch // heads) ** (-0.5))).astype(BF16)
    gs[...] = jax.nn.sigmoid(mm(normed, wg_ref[...]))
    for q in range(n // per):
        vm[:, q * 128 : (q + 1) * 128] = pick(
            [lx[q * per + k, :, span:].astype(F32) for k in range(per)]
        )

    ring(rz, rz_s, rz_r, 4, 5, turn, land_right)
    for q in range(wide // 128):
        rt[q * 128 : (q + 1) * 128, :] = rf[:, q * 128 : (q + 1) * 128].T

    def reorder(d, _):
        rt2[pl.ds(pl.multiple_of(d * res, res), res), :] = rt[
            pl.ds(d, res, stride=opm), :
        ].astype(BF16)
        return 0

    lax.fori_loop(0, opm, reorder, 0)

    def half_left(i, k):
        block = lz[i, k].astype(F32)
        at = pl.ds(pl.multiple_of(i * ns, ns), ns)
        lf[k, at, :] = block

    def share_left(t, _):
        i = col_peer(t)
        lz_copy(i, a).wait_recv()
        lf_copy(i, core).start()
        half_left(i, core)
        return 0

    half_left(a, core)
    lax.fori_loop(1, n, share_left, 0)

    def land_left(t, _):
        i = col_peer(t)
        lf_copy(i, 1 - core).wait_recv()
        half_left(i, 1 - core)
        return 0

    lax.fori_loop(0, n, land_left, 0)

    groups = res // per
    for g in range(groups):
        at = (g % (groups // 2)) * 128
        lb[g] = lf[g // (groups // 2), :, at : at + 128].astype(BF16)

    def outer(g, _):
        block = mm(rt2[...], lb[g]).astype(BF16)
        for d in range(opm):
            lhs[pl.ds(pl.multiple_of(g * res, res), res), d * 128 : (d + 1) * 128] = block[
                d * res : (d + 1) * res
            ]
        return 0

    lax.fori_loop(0, groups, outer, 0)
    upd[...] = mm(lhs[...], bd[...])

    def pass_rows(first, last):
        for i in x_blocks(first, last):
            x1_copy(i, b, core).wait_recv()
            if (first, last) == (1, 2):
                continue
            xf_copy(i).start()

    pass_rows(1, 2)
    x_on()
    for i in x_blocks(1, 2):
        xf_copy(i).start()
    count = mm(rf[:, wide:].T.astype(BF16), lf[0, :, span:].astype(BF16))
    inverse = 1.0 / count[:res]
    loads[3].wait()
    step = 8
    for at in range(0, res, step):
        block = jnp.concatenate(
            [
                upd[i // per * res : (i // per + 1) * res, i % per * 128 : (i % per + 1) * 128]
                * inverse[:, i : i + 1]
                for i in range(at, at + step)
            ],
            axis=0,
        )
        old = pair_ref[at : at + step].reshape(step * res, cz).astype(F32)
        fresh = (old + block).astype(BF16)
        pair_out[at : at + step] = fresh.reshape(step, res, cz)
        pn[at * res : (at + step) * res, :] = row_norm(fresh.astype(F32)).astype(BF16)
    tz[a] = mm_nt(pbw_ref[...], pn[...])

    spread(tz, tz_s, tz_r, 0, 3)
    store = pltpu.make_async_copy(pair_out, pair_hbm_out, store_sem.at[0])
    store.start()

    def pass_bias(i):
        @pl.when(i != b)
        def _():
            bx_copy(b, i).start()

        @pl.when(i == b)
        def _():
            bx[b] = tz[i]

    pass_bias(a)
    ring(tz, tz_s, tz_r, 3, 1, min(3, turn), pass_bias)
    pass_rows(3, across)
    x1_copy(partner, b, core).wait_recv()
    in_part(partner).wait_recv()

    def land_rows(t, _):
        in_part(row_peer(t)).wait_recv()
        return 0

    lax.fori_loop(2, n, land_rows, 0)
    head_lane = lax.broadcasted_iota(jnp.int32, (res, ch), 1) // (ch // heads)

    loads[4].wait()
    loads[5].wait()

    def score(s, _):
        x = rows[s].reshape(n * res, ch)
        key = mm(x, wk_ref[...]).astype(BF16)
        kv[s] = mm(x, wv_ref[...]).astype(BF16)
        q = qs[pl.ds(pl.multiple_of(s * res, res), res), :].astype(F32)
        query = jnp.concatenate(
            [jnp.where(head_lane == h, q, 0.0) for h in range(heads)], axis=0
        ).astype(BF16)
        sc[s] = mm_nt(query, key)
        return 0

    lax.fori_loop(0, half, score, 0)
    ring(tz, tz_s, tz_r, 3, 4, min(6, turn), pass_bias)
    lax.fori_loop(half, ns, score, 0)

    def drain(t, _):
        lx_copy(b, (b + t) % n).wait_send()
        lz_copy(a, (a + t) % n).wait_send()
        return 0

    lax.fori_loop(1, n, drain, 0)

    def drain_left(t, _):
        lf_copy(t, core).wait_send()
        return 0

    lax.fori_loop(0, n, drain_left, 0)
    ring_sent(rz, rz_s, rz_r, 4)
    x_first(wait=True)
    x_on(wait=True)
    x1_copy(b, partner, 1 - core).wait_send()

    def drain_rows(t, _):
        xf_copy(row_peer(t)).wait_send()
        return 0

    lax.fori_loop(2, n, drain_rows, 0)
    xf_copy(b).wait_send()
    store.wait()
    for load in loads[6:]:
        load.wait()
    ring(tz, tz_s, tz_r, 3, 7, turn, pass_bias)

    for q in range(n // per):
        for k in range(per):
            i = q * per + k

            @pl.when(i != b)
            def _():
                bx_copy(i, b).wait_recv()

        for v in range(res // per):
            cut = [bx[q * per + k, :, v * 128 : (v + 1) * 128] for k in range(per)]
            turned = [cut[0]] + [pltpu.roll(cut[k], opm * k, 1) for k in range(1, per)]
            for m in range(per):
                mixed = pick([turned[(k - m) % per] for k in range(per)])
                if m:
                    mixed = pltpu.roll(mixed, 128 - opm * m, 1)
                i = v * per + m
                bi[q, i * heads : (i + 1) * heads, :] = mixed
        for h in range(heads):
            bh[h * res : (h + 1) * res, q * 128 : (q + 1) * 128] = bi[
                q, pl.ds(h, res, stride=heads), :
            ]

    def attend(s, _):
        valid = vm[pl.ds(s, 1), :]
        scores = jnp.where(valid > 0, sc[s] + bh[...], -1000000000.0)
        top = jnp.max(scores, axis=-1, keepdims=True)
        raw = jnp.exp(scores - top)
        mass = jnp.sum(raw, axis=-1, keepdims=True)
        mixed = mm(raw.astype(BF16), kv[s]) / mass
        out = mixed[:res]
        for h in range(1, heads):
            out = jnp.where(head_lane == h, mixed[h * res : (h + 1) * res], out)
        at = pl.ds(pl.multiple_of(s * res, res), res)
        gated[at, :] = (out * gs[at, :]).astype(BF16)
        return 0

    lax.fori_loop(0, ns, attend, 0)

    middle = state_ref[...].reshape(ns * res, ch).astype(F32) + mm(gated[...], wo_ref[...])
    hidden = jnp.maximum(mm(row_norm(middle).astype(BF16), up_ref[...]), 0.0).astype(BF16)
    final = middle + mm(hidden, down_ref[...])
    msa_out[...] = final.astype(BF16).reshape(ns, res, ch)
    store = pltpu.make_async_copy(msa_out, msa_hbm_out, store_sem.at[1])
    store.start()
    ring_sent(tz, tz_s, tz_r, 3)

    def drain_bias(t, _):
        bx_copy(b, (b + t) % n).wait_send()
        return 0

    lax.fori_loop(1, n, drain_bias, 0)
    store.wait()


def per_device(n, *args):
    state, pair, mask, left, _, _, pbw = args[:7]
    ns, res, ch = state.shape
    opm, heads, cz = left.shape[1], pbw.shape[1], pair.shape[2]
    args = args[:3] + (left.T, args[4].T, args[5], pbw.T) + args[7:]
    wide = res * opm
    span = wide // 2
    per = 128 // opm
    groups = res // per
    keys = n * res
    dma = pltpu.SemaphoreType.DMA((n,))
    vmem = pl.BlockSpec(memory_space=pltpu.VMEM)
    far = pl.BlockSpec(memory_space=pl.ANY)
    near = (0, 2, 3, 4, 6)
    order = (1, 5, 7, 8, 9, 10, 11, 12, 13)
    return tuple(
        pl.pallas_call(
            functools.partial(body, n),
            out_shape=(
                jax.ShapeDtypeStruct(state.shape, BF16),
                jax.ShapeDtypeStruct(pair.shape, BF16),
            ),
            in_specs=[vmem if k in near else far for k in range(len(args))],
            out_specs=(far, far),
            scratch_shapes=[pltpu.VMEM(args[k].shape, args[k].dtype) for k in order]
            + [
                pltpu.VMEM(pair.shape, BF16),
                pltpu.VMEM(state.shape, BF16),
                pltpu.SemaphoreType.DMA((len(order),)),
                pltpu.SemaphoreType.DMA((2,)),
                pltpu.VMEM((ns, n, res, ch), BF16),
                pltpu.VMEM((ch // 128, ns * res, 128), F32),
                pltpu.VMEM((2, ns, span + 128), BF16),
                pltpu.VMEM((n, ns, span + 128), BF16),
                pltpu.VMEM((n, 2, ns, span + 128), BF16),
                pltpu.VMEM((n, ns, wide + 128), BF16),
                pltpu.VMEM((n, heads, res * res), F32),
                pltpu.VMEM((n, heads, res * res), F32),
                pltpu.VMEM((2, n * ns, span + 128), F32),
                pltpu.VMEM((n * ns, wide + 128), F32),
                pltpu.VMEM((wide, n * ns), F32),
                pltpu.VMEM((wide, n * ns), BF16),
                pltpu.VMEM((groups, n * ns, 128), BF16),
                pltpu.VMEM((opm * opm, cz), F32),
                pltpu.VMEM((opm * 128, per * cz), BF16),
                pltpu.VMEM((groups * res, opm * 128), BF16),
                pltpu.VMEM((groups * res, per * cz), F32),
                pltpu.VMEM((res * res, cz), BF16),
                pltpu.VMEM((keys // 128, res * heads, 128), F32),
                pltpu.VMEM((heads * res, keys), F32),
                pltpu.VMEM((ns, keys, ch), BF16),
                pltpu.VMEM((ns, heads * res, keys), F32),
                pltpu.VMEM((ns * res, ch), BF16),
                pltpu.VMEM((ns * res, ch), F32),
                pltpu.VMEM((ns, keys), F32),
                pltpu.VMEM((ns * res, ch), BF16),
            ]
            + [dma] * 17,
            compiler_params=pltpu.CompilerParams(collective_id=0, has_side_effects=True),
        )(*args)
    )


def solution(mesh):
    spec = P(("groups", "aa"), "ba", None)
    return jax.shard_map(
        functools.partial(per_device, mesh.shape["ba"]),
        mesh=mesh,
        in_specs=(spec, spec, P(("groups", "aa"), "ba")) + (P(),) * 11,
        out_specs=(spec, spec),
        check_vma=False,
    )
```

```python
import functools

import jax
import jax.numpy as jnp
from jax import lax
from jax.experimental import pallas as pl
from jax.experimental.pallas import tpu as pltpu
from jax.sharding import PartitionSpec as P

F32 = jnp.float32
BF16 = jnp.bfloat16
NT = (((1,), (1,)), ((), ()))


def mm(x, y):
    return jnp.dot(x, y, preferred_element_type=F32)


def mm_nt(x, y):
    return lax.dot_general(x, y, NT, preferred_element_type=F32)


def row_norm(values):
    center = values - jnp.mean(values, axis=-1, keepdims=True)
    spread = jnp.mean(center * center, axis=-1, keepdims=True)
    return center * lax.rsqrt(spread + 1e-05)


def near_to_far(t):
    return ((t + 1) // 2) * (2 * (t % 2) - 1)


def body(
    n,
    state_ref,
    pair_hbm,
    mask_ref,
    left_ref,
    right_ref,
    outer_hbm,
    pbw_ref,
    wq_hbm,
    wk_hbm,
    wv_hbm,
    wg_hbm,
    wo_hbm,
    up_hbm,
    down_hbm,
    msa_hbm_out,
    pair_hbm_out,
    pair_ref,
    outer_ref,
    wq_ref,
    wk_ref,
    wv_ref,
    wg_ref,
    wo_ref,
    up_ref,
    down_ref,
    pair_out,
    msa_out,
    load_sem,
    store_sem,
    rows,
    nf,
    ls,
    lx,
    lz,
    rz,
    tz,
    bx,
    kt,
    ka,
    sel,
    expand,
    rt,
    rt2,
    lb,
    wf,
    bd,
    lhs,
    upd,
    pn,
    bi,
    bh,
    kv,
    sc,
    qs,
    gs,
    vm,
    gated,
    lx_s,
    lz_s,
    lf_s,
    ka_s,
    rz_s,
    x_s,
    tz_s,
    bx_s,
    lx_r,
    lz_r,
    tz_r,
    rz_r,
    x1_r,
    bx_r,
    lf_r,
    ka_r,
    xf_r,
):
    a = lax.axis_index("aa")
    b = lax.axis_index("ba")
    core = b % 2
    chip = b // 2
    chips = n // 2
    partner = chip * 2 + 1 - core
    ns = state_ref.shape[0]
    res = state_ref.shape[1]
    ch = state_ref.shape[2]
    half = ns // 2
    opm = left_ref.shape[0]
    cz = pair_ref.shape[2]
    heads = pbw_ref.shape[0]
    wide = res * opm
    per = 128 // opm
    parts = 4
    mine = b % parts
    span = wide // parts

    hbm = (outer_hbm, wq_hbm, wg_hbm, pair_hbm, wk_hbm, wv_hbm, wo_hbm, up_hbm, down_hbm)
    local = (outer_ref, wq_ref, wg_ref, pair_ref, wk_ref, wv_ref, wo_ref, up_ref, down_ref)
    loads = [
        pltpu.make_async_copy(src, dst, load_sem.at[k])
        for k, (src, dst) in enumerate(zip(hbm, local))
    ]

    def row_peer(t):
        c = (chip + near_to_far(t // 2) + chips) % chips
        return c * 2 + t % 2

    def col_peer(t):
        return (a + near_to_far(t) + n) % n

    barrier = pltpu.get_barrier_semaphore()

    def greet(t, _):
        pl.semaphore_signal(
            barrier, inc=1, device_id={"ba": (b + t) % n}, device_id_type=pl.DeviceIdType.MESH
        )
        pl.semaphore_signal(
            barrier, inc=1, device_id={"aa": (a + t) % n}, device_id_type=pl.DeviceIdType.MESH
        )
        return 0

    lax.fori_loop(1, n, greet, 0)

    for load in loads:
        load.start()

    state = state_ref[...].reshape(ns * res, ch).astype(F32)
    normed = row_norm(state).astype(BF16)
    rows[:, b] = normed.reshape(ns, res, ch)
    for q in range(ch // 128):
        nf[q] = normed[:, q * 128 : (q + 1) * 128].astype(F32)
    by_res = jnp.concatenate(
        [
            jnp.concatenate(
                [nf[q, pl.ds(r, ns, stride=res), :] for r in range(res)], axis=0
            ).astype(BF16)
            for q in range(ch // 128)
        ],
        axis=1,
    )
    lane = lax.broadcasted_iota(jnp.int32, (opm, 128), 1)
    line = lax.broadcasted_iota(jnp.int32, (opm, 128), 0)
    rep = jnp.where(lane % opm == line, 1.0, 0.0).astype(BF16)
    lane_t = lax.broadcasted_iota(jnp.int32, (128, opm), 1)
    line_t = lax.broadcasted_iota(jnp.int32, (128, opm), 0)
    rep_t = jnp.where(line_t % opm == lane_t, 1.0, 0.0).astype(BF16)
    seg = lax.broadcasted_iota(jnp.int32, (ns, 128), 1) // opm
    keep = mask_ref[...].astype(F32).astype(BF16)
    lane_w = lax.broadcasted_iota(jnp.int32, (res, wide), 1) // opm
    line_w = lax.broadcasted_iota(jnp.int32, (res, wide), 0)
    keep_wide = mm(keep, jnp.where(lane_w == line_w, 1.0, 0.0).astype(BF16))
    keep_rep = mm(keep, rep).astype(BF16)

    def pick(parts):
        out = parts[0]
        for k in range(1, per):
            out = jnp.where(seg == k, parts[k], out)
        return out

    def factor(w_ref):
        y = mm_nt(by_res, mm(rep_t, w_ref[...]).astype(BF16))
        cols = [
            pick([y[(q * per + k) * ns : (q * per + k + 1) * ns] for k in range(per)])
            for q in range(res // per)
        ]
        return (jnp.concatenate(cols, axis=1) * keep_wide).astype(BF16)

    left = factor(left_ref)
    for k in range(parts):
        ls[k, :, :span] = left[:, k * span : (k + 1) * span]
        ls[k, :, span:] = keep_rep
    lx[b] = ls[mine]
    rz[a, :, :wide] = factor(right_ref)
    rz[a, :, wide:] = keep_rep

    pl.semaphore_wait(barrier, 2 * (n - 1))

    def to_row(buf, src, i, who, ss, rs):
        return pltpu.make_async_remote_copy(
            src_ref=src,
            dst_ref=buf,
            send_sem=ss,
            recv_sem=rs.at[i],
            device_id={"ba": who},
            device_id_type=pl.DeviceIdType.MESH,
        )

    def to_col(buf, src, i, who, ss, rs):
        return pltpu.make_async_remote_copy(
            src_ref=src,
            dst_ref=buf,
            send_sem=ss,
            recv_sem=rs.at[i],
            device_id={"aa": who},
            device_id_type=pl.DeviceIdType.MESH,
        )

    def lx_copy(i, who):
        return to_row(lx.at[i], ls.at[who % parts], i, who, lx_s, lx_r)

    def lz_copy(i, who):
        return to_col(lz.at[i, mine], lx.at[who, :, pl.ds(0, span)], i, who, lz_s, lz_r)

    def lf_copy(i, q, k, src=None):
        part = lz.at[i, q]
        return pltpu.make_async_remote_copy(
            src_ref=part if src is None else src,
            dst_ref=part,
            send_sem=lf_s,
            recv_sem=lf_r,
            device_id={"ba": b - mine + (mine + k) % parts},
            device_id_type=pl.DeviceIdType.MESH,
        )

    def ka_copy(who):
        return pltpu.make_async_remote_copy(
            src_ref=kt,
            dst_ref=ka,
            send_sem=ka_s,
            recv_sem=ka_r,
            device_id={"ba": who},
            device_id_type=pl.DeviceIdType.MESH,
        )

    def bx_copy(i, who):
        return pltpu.make_async_remote_copy(
            src_ref=tz.at[who],
            dst_ref=bx.at[i],
            send_sem=bx_s,
            recv_sem=bx_r.at[i // per],
            device_id={"ba": who},
            device_id_type=pl.DeviceIdType.MESH,
        )

    turn = n // 2

    def hop(buf, ss, rs, d, step, way):
        i = (a + n - way * d) % n
        part = buf.at[i]
        return pltpu.make_async_remote_copy(
            src_ref=part,
            dst_ref=part,
            send_sem=ss,
            recv_sem=rs(i, d + step, way),
            device_id={"aa": (a + n + way * step) % n},
            device_id_type=pl.DeviceIdType.MESH,
        )

    def spread(buf, ss, rs, d, reach):
        def one(step, way):
            hop(buf, ss, rs, d, step, way).start()

        for step in range(min(reach, turn - d), 0, -1):
            for way in (1, -1):
                if d + step < turn:
                    one(step, way)
                else:
                    pl.when(core == (1 - way) // 2)(functools.partial(one, step, way))

    def ring(buf, ss, rs, reach, first, last, landed):
        for d in range(first, last + 1):
            for way in (1, -1):
                if d < turn or way > 0:
                    hop(buf, ss, rs, d, 0, way).wait_recv()
            if d % reach == 0:
                spread(buf, ss, rs, d, reach)
            for way in (1, -1):
                if d < turn or way > 0:
                    landed((a + n - way * d) % n)

    def tz_at(i, d, way):
        return tz_r.at[i]

    reach = 4
    passed = [d for d in range(reach, turn, reach)]

    def rz_at(i, d, way):
        if d in passed:
            return rz_r.at[1 + 2 * passed.index(d) + (1 - way) // 2]
        return rz_r.at[0]

    def all_sent(sem, part):
        pltpu.make_async_remote_copy(
            src_ref=part,
            dst_ref=part,
            send_sem=sem,
            recv_sem=sem,
            device_id={"ba": partner},
            device_id_type=pl.DeviceIdType.MESH,
        ).wait_send()

    def all_here(sem, part):
        pltpu.make_async_remote_copy(
            src_ref=part,
            dst_ref=part,
            send_sem=sem,
            recv_sem=sem,
            device_id={"ba": partner},
            device_id_type=pl.DeviceIdType.MESH,
        ).wait_recv()

    across = chips // 2

    def x_to(i, c, step, way, d):
        part = rows.at[pl.ds(half * c, half), i]
        who = ((chip + chips + way * step) % chips) * 2 + c
        return pltpu.make_async_remote_copy(
            src_ref=part,
            dst_ref=part,
            send_sem=x_s,
            recv_sem=x1_r.at[(d + 1) // 2],
            device_id={"ba": who},
            device_id_type=pl.DeviceIdType.MESH,
        )

    def x_first():
        def one(step, way, c):
            x_to(b, c, step, way, step).start()

        for step in range(min(2, across), 0, -1):
            for way in (1, -1):
                for c in range(2):
                    if step < across:
                        one(step, way, c)
                    else:
                        pl.when(core == (1 - way) // 2)(functools.partial(one, step, way, c))

    def x_on():
        for step in range(min(2, across - 2), 0, -1):
            for way in (1, -1):
                for c in range(2):
                    if 2 + step < across or c == (1 - way) // 2:
                        i = ((chip + chips - 2 * way) % chips) * 2 + c
                        x_to(i, core, step, way, 2 + step).start()

    def x_blocks(first, last):
        return [
            ((chip + chips - way * d) % chips) * 2 + c
            for d in range(first, min(last, across) + 1)
            for way in (1, -1)
            if d < across or way > 0
            for c in range(2)
        ]

    def xf_copy(i, c, sem):
        part = rows.at[pl.ds(half * c, half), i]
        return pltpu.make_async_remote_copy(
            src_ref=part,
            dst_ref=part,
            send_sem=x_s,
            recv_sem=sem,
            device_id={"ba": partner},
            device_id_type=pl.DeviceIdType.MESH,
        )

    def start_l_off(t, _):
        lx_copy(b, row_peer(n - 1 - t)).start()
        return 0

    lx_copy(b, partner).start()
    lax.fori_loop(0, n - 2, start_l_off, 0)
    spread(rz, rz_s, rz_at, 0, reach)
    x_first()
    xf_copy(b, 1 - core, xf_r).start()
    xf_copy(b, core, xf_r).start()

    loads[0].wait()
    wf[...] = outer_ref[...].astype(F32)

    def build(d, _):
        w = wf[pl.ds(d, opm, stride=opm), :].astype(BF16)
        zero = jnp.zeros_like(w)
        for k in range(per):
            bd[pl.ds(d * 128 + k * opm, opm), :] = jnp.concatenate(
                [w if m == k else zero for m in range(per)], axis=1
            )
        return 0

    lax.fori_loop(0, opm, build, 0)

    lane_e = lax.broadcasted_iota(jnp.int32, (128, res * res), 1)
    line_e = lax.broadcasted_iota(jnp.int32, (128, res * res), 0)
    sel[...] = jnp.where(lane_e == line_e * res, 1.0, 0.0).astype(BF16)
    expand[...] = jnp.where(lane_e // res == line_e, 1.0, 0.0).astype(BF16)

    def pass_left(t, _):
        i = row_peer(t)

        @pl.when(i != b)
        def _():
            lx_copy(i, b).wait_recv()

        @pl.when(i != a)
        def _():
            lz_copy(a, i).start()

        @pl.when(i == a)
        def _():
            lz[a, mine] = lx[i, :, :span]
            for k in range(1, parts):
                lf_copy(a, mine, k, lx.at[i, :, pl.ds(0, span)]).start()

        return 0

    def nothing(i):
        pass

    lax.fori_loop(0, n * 5 // 8, pass_left, 0)
    for d in passed:
        for way in (1, -1):
            hop(rz, rz_s, rz_at, d, 0, way).wait_recv()
        spread(rz, rz_s, rz_at, d, reach)
    lax.fori_loop(n * 5 // 8, n, pass_left, 0)

    loads[1].wait()
    loads[2].wait()
    qs[...] = (mm(normed, wq_ref[...]) * ((ch // heads) ** (-0.5))).astype(BF16)
    gs[...] = jax.nn.sigmoid(mm(normed, wg_ref[...]))
    for q in range(n // per):
        vm[:, q * 128 : (q + 1) * 128] = pick(
            [lx[q * per + k, :, span:].astype(F32) for k in range(per)]
        )

    def share_left(t, _):
        i = col_peer(t)
        lz_copy(i, a).wait_recv()
        for k in range(1, parts):
            lf_copy(i, mine, k).start()
        return 0

    lax.fori_loop(1, n, share_left, 0)
    all_here(rz_r.at[0], rz.at[pl.ds(0, n - 1 - 2 * len(passed))])
    for q in range(wide // 128):
        block = rz[:, :, q * 128 : (q + 1) * 128].astype(F32).reshape(n * ns, 128)
        rt[q * 128 : (q + 1) * 128, :] = block.T
    kt[...] = rz[:, :, wide:].astype(F32).reshape(n * ns, 128).T[:res].astype(BF16)

    def send_keep(t, _):
        ka_copy((b + t) % n).start()
        return 0

    @pl.when(a == b)
    def _():
        lax.fori_loop(1, n, send_keep, 0)
        ka[...] = kt[...]

    def reorder(d, _):
        rt2[pl.ds(pl.multiple_of(d * res, res), res), :] = rt[
            pl.ds(d, res, stride=opm), :
        ].astype(BF16)
        return 0

    lax.fori_loop(0, opm, reorder, 0)


    all_here(lf_r, lz.at[:, pl.ds(0, parts - 1)])

    def pass_rows(first, last, then):
        blocks = x_blocks(first, last)
        if blocks:
            many = rows.at[pl.ds(0, half), pl.ds(0, len(blocks))]
            all_here(x1_r.at[(last + 1) // 2], many)
        then()
        for i in blocks:
            xf_copy(i, core, xf_r).start()

    pass_rows(1, 2, x_on)

    groups = res // per
    for g in range(groups // 2):
        at = g * 256 % span
        block = lz[:, g * 256 // span, :, at : at + 256].astype(F32)
        lb[g] = block.reshape(n * ns, 256).astype(BF16)

    def outer(g, _):
        block = mm(rt2[...], lb[g]).astype(BF16)
        for k in range(2):
            at = pl.ds(pl.multiple_of((2 * g + k) * res, res), res)
            for d in range(opm):
                lhs[at, d * 128 : (d + 1) * 128] = block[
                    d * res : (d + 1) * res, k * 128 : (k + 1) * 128
                ]
        return 0

    lax.fori_loop(0, groups // 2, outer, 0)
    upd[...] = mm(lhs[...], bd[...])


    @pl.when(a != b)
    def _():
        ka_copy(a).wait_recv()

    inverse = 1.0 / mm_nt(kt[...], ka[...])
    loads[3].wait()
    step = 8
    for at in range(0, res, step):
        block = jnp.concatenate(
            [
                upd[i // per * res : (i // per + 1) * res, i % per * 128 : (i % per + 1) * 128]
                * inverse[:, i : i + 1]
                for i in range(at, at + step)
            ],
            axis=0,
        )
        old = pair_ref[at : at + step].reshape(step * res, cz).astype(F32)
        fresh = (old + block).astype(BF16)
        pair_out[at : at + step] = fresh.reshape(step, res, cz)
        pn[at * res : (at + step) * res, :] = row_norm(fresh.astype(F32)).astype(BF16)
    tile = mm_nt(pbw_ref[...], pn[...])
    lane_t = lax.broadcasted_iota(jnp.int32, (heads, 128), 1)
    base = []
    for v in range(res // per):
        top = tile[:, v * 128 : (v + 1) * 128]
        by = 1
        while by < res:
            other = jnp.where(
                lane_t // by % 2 == 1, pltpu.roll(top, by, 1), pltpu.roll(top, 128 - by, 1)
            )
            top = jnp.maximum(top, other)
            by *= 2
        base.append(top)
    base = jnp.concatenate(base, axis=1).astype(BF16)
    tz[a, :, : res * res] = (tile - base.astype(F32)).astype(BF16)
    tz[a, :, res * res :] = mm_nt(base, sel[...]).astype(BF16)
    spread(tz, tz_s, tz_at, 0, 4)
    store = pltpu.make_async_copy(pair_out, pair_hbm_out, store_sem.at[0])
    store.start()

    def pass_bias(i):
        @pl.when(i != b)
        def _():
            bx_copy(b, i).start()

        @pl.when(i == b)
        def _():
            bx[b] = tz[i]

    pass_bias(a)
    ring(tz, tz_s, tz_at, 4, 1, min(4, turn), pass_bias)
    pass_rows(3, 4, lambda: None)
    all_here(xf_r, rows.at[pl.ds(0, half), pl.ds(0, n)])
    head_lane = lax.broadcasted_iota(jnp.int32, (res, ch), 1) // (ch // heads)

    loads[4].wait()
    loads[5].wait()

    def score(s, _):
        x = rows[s].reshape(n * res, ch)
        key = mm(x, wk_ref[...]).astype(BF16)
        kv[s] = mm(x, wv_ref[...]).astype(BF16)
        q = qs[pl.ds(pl.multiple_of(s * res, res), res), :].astype(F32)
        query = jnp.concatenate(
            [jnp.where(head_lane == h, q, 0.0) for h in range(heads)], axis=0
        ).astype(BF16)
        sc[s] = mm_nt(query, key)
        return 0

    lax.fori_loop(0, ns, score, 0)
    ring(tz, tz_s, tz_at, 4, 5, turn, pass_bias)

    others = pl.ds(0, n - 1)
    all_sent(lx_s, lx.at[others])
    all_sent(lz_s, lz.at[others, 0])
    all_sent(lf_s, lz.at[:, pl.ds(0, parts - 1)])
    all_sent(rz_s, rz.at[others])
    all_sent(x_s, rows.at[:, others])

    @pl.when(a == b)
    def _():
        all_sent(ka_s, pn.at[pl.ds(0, (n - 1) * res)])

    store.wait()
    for load in loads[6:]:
        load.wait()

    for q in range(n // per):
        @pl.when(b // per == q)
        def _():
            all_here(bx_r.at[q], bx.at[pl.ds(0, per - 1)])

        @pl.when(b // per != q)
        def _():
            all_here(bx_r.at[q], bx.at[pl.ds(0, per)])

        base = bx[q * per : (q + 1) * per, :, res * res :].astype(F32)
        base = mm(base.reshape(per * heads, 128).astype(BF16), expand[...])
        for v in range(res // per):
            cols = slice(v * 128, (v + 1) * 128)
            cut = [
                bx[q * per + k, :, cols].astype(F32) + base[k * heads : (k + 1) * heads, cols]
                for k in range(per)
            ]
            turned = [cut[0]] + [pltpu.roll(cut[k], opm * k, 1) for k in range(1, per)]
            for m in range(per):
                mixed = pick([turned[(k - m) % per] for k in range(per)])
                if m:
                    mixed = pltpu.roll(mixed, 128 - opm * m, 1)
                i = v * per + m
                bi[q, i * heads : (i + 1) * heads, :] = mixed
        for h in range(heads):
            bh[h * res : (h + 1) * res, q * 128 : (q + 1) * 128] = bi[
                q, pl.ds(h, res, stride=heads), :
            ]

    def attend(s, _):
        valid = vm[pl.ds(s, 1), :]
        scores = jnp.where(valid > 0, sc[s] + bh[...], -1000000000.0)
        top = jnp.max(scores, axis=-1, keepdims=True)
        raw = jnp.exp(scores - top)
        mass = jnp.sum(raw, axis=-1, keepdims=True)
        mixed = mm(raw.astype(BF16), kv[s]) / mass
        out = mixed[:res]
        for h in range(1, heads):
            out = jnp.where(head_lane == h, mixed[h * res : (h + 1) * res], out)
        at = pl.ds(pl.multiple_of(s * res, res), res)
        gated[at, :] = (out * gs[at, :]).astype(BF16)
        return 0

    lax.fori_loop(0, ns, attend, 0, unroll=2)

    middle = state_ref[...].reshape(ns * res, ch).astype(F32) + mm(gated[...], wo_ref[...])
    hidden = jnp.maximum(mm(row_norm(middle).astype(BF16), up_ref[...]), 0.0).astype(BF16)
    final = middle + mm(hidden, down_ref[...])
    msa_out[...] = final.astype(BF16).reshape(ns, res, ch)
    store = pltpu.make_async_copy(msa_out, msa_hbm_out, store_sem.at[1])
    store.start()
    all_sent(tz_s, tz.at[others])
    all_sent(bx_s, bx.at[others])
    store.wait()


def per_device(n, *args):
    state, pair, mask, left, _, _, pbw = args[:7]
    ns, res, ch = state.shape
    opm, heads, cz = left.shape[1], pbw.shape[1], pair.shape[2]
    args = args[:3] + (left.T, args[4].T, args[5], pbw.T) + args[7:]
    wide = res * opm
    parts = 4
    span = wide // parts
    per = 128 // opm
    groups = res // per
    keys = n * res
    dma = pltpu.SemaphoreType.DMA((n,))
    vmem = pl.BlockSpec(memory_space=pltpu.VMEM)
    far = pl.BlockSpec(memory_space=pl.ANY)
    near = (0, 2, 3, 4, 6)
    order = (1, 5, 7, 8, 9, 10, 11, 12, 13)
    return tuple(
        pl.pallas_call(
            functools.partial(body, n),
            out_shape=(
                jax.ShapeDtypeStruct(state.shape, BF16),
                jax.ShapeDtypeStruct(pair.shape, BF16),
            ),
            in_specs=[vmem if k in near else far for k in range(len(args))],
            out_specs=(far, far),
            scratch_shapes=[pltpu.VMEM(args[k].shape, args[k].dtype) for k in order]
            + [
                pltpu.VMEM(pair.shape, BF16),
                pltpu.VMEM(state.shape, BF16),
                pltpu.SemaphoreType.DMA((len(order),)),
                pltpu.SemaphoreType.DMA((2,)),
                pltpu.VMEM((ns, n, res, ch), BF16),
                pltpu.VMEM((ch // 128, ns * res, 128), F32),
                pltpu.VMEM((parts, ns, span + 128), BF16),
                pltpu.VMEM((n, ns, span + 128), BF16),
                pltpu.VMEM((n, parts, ns, span), BF16),
                pltpu.VMEM((n, ns, wide + 128), BF16),
                pltpu.VMEM((n, heads, res * res + 128), BF16),
                pltpu.VMEM((n, heads, res * res + 128), BF16),
                pltpu.VMEM((res, n * ns), BF16),
                pltpu.VMEM((res, n * ns), BF16),
                pltpu.VMEM((128, res * res), BF16),
                pltpu.VMEM((128, res * res), BF16),
                pltpu.VMEM((wide, n * ns), F32),
                pltpu.VMEM((wide, n * ns), BF16),
                pltpu.VMEM((groups // 2, n * ns, 256), BF16),
                pltpu.VMEM((opm * opm, cz), F32),
                pltpu.VMEM((opm * 128, per * cz), BF16),
                pltpu.VMEM((groups * res, opm * 128), BF16),
                pltpu.VMEM((groups * res, per * cz), F32),
                pltpu.VMEM((res * res, cz), BF16),
                pltpu.VMEM((keys // 128, res * heads, 128), F32),
                pltpu.VMEM((heads * res, keys), F32),
                pltpu.VMEM((ns, keys, ch), BF16),
                pltpu.VMEM((ns, heads * res, keys), F32),
                pltpu.VMEM((ns * res, ch), BF16),
                pltpu.VMEM((ns * res, ch), F32),
                pltpu.VMEM((ns, keys), F32),
                pltpu.VMEM((ns * res, ch), BF16),
            ]
            + [pltpu.SemaphoreType.DMA] * 8
            + [dma] * 3
            + [pltpu.SemaphoreType.DMA((3,))] * 2
            + [pltpu.SemaphoreType.DMA((n // per,))]
            + [pltpu.SemaphoreType.DMA] * 3,
            compiler_params=pltpu.CompilerParams(collective_id=0, has_side_effects=True),
        )(*args)
    )


def solution(mesh):
    spec = P(("groups", "aa"), "ba", None)
    return jax.shard_map(
        functools.partial(per_device, mesh.shape["ba"]),
        mesh=mesh,
        in_specs=(spec, spec, P(("groups", "aa"), "ba")) + (P(),) * 11,
        out_specs=(spec, spec),
        check_vma=False,
    )
```

```python
import functools

import jax
import jax.numpy as jnp
from jax import lax
from jax.experimental import pallas as pl
from jax.experimental.pallas import tpu as pltpu
from jax.sharding import PartitionSpec as P

F32 = jnp.float32
BF16 = jnp.bfloat16
NT = (((1,), (1,)), ((), ()))


def mm(x, y):
    return jnp.dot(x, y, preferred_element_type=F32)


def mm_nt(x, y):
    return lax.dot_general(x, y, NT, preferred_element_type=F32)


def row_norm(values):
    center = values - jnp.mean(values, axis=-1, keepdims=True)
    spread = jnp.mean(center * center, axis=-1, keepdims=True)
    return center * lax.rsqrt(spread + 1e-05)


def near_to_far(t):
    return ((t + 1) // 2) * (2 * (t % 2) - 1)


def body(
    n,
    state_hbm,
    pair_hbm,
    mask_hbm,
    left_hbm,
    right_hbm,
    outer_hbm,
    pbw_hbm,
    wq_hbm,
    wk_hbm,
    wv_hbm,
    wg_hbm,
    wo_hbm,
    up_hbm,
    down_hbm,
    msa_hbm_out,
    pair_hbm_out,
    state_ref,
    mask_ref,
    left_ref,
    right_ref,
    pbw_ref,
    pair_ref,
    outer_ref,
    wq_ref,
    wk_ref,
    wv_ref,
    wg_ref,
    wo_ref,
    up_ref,
    down_ref,
    pair_out,
    msa_out,
    load_sem,
    store_sem,
    rows,
    nf,
    ls,
    lx,
    lz,
    rz,
    tz,
    bx,
    kt,
    ka,
    sel,
    expand,
    rt,
    rt2,
    lb,
    wf,
    bd,
    lhs,
    upd,
    pn,
    bi,
    bh,
    kv,
    sc,
    qs,
    gs,
    vm,
    gated,
    lx_s,
    lz_s,
    lf_s,
    ka_s,
    rz_s,
    x_s,
    tz_s,
    bx_s,
    lx_r,
    lz_r,
    tz_r,
    rz_r,
    x1_r,
    bx_r,
    lf_r,
    ka_r,
    xf_r,
):
    a = lax.axis_index("aa")
    b = lax.axis_index("ba")
    core = b % 2
    chip = b // 2
    chips = n // 2
    partner = chip * 2 + 1 - core
    ns = state_ref.shape[0]
    res = state_ref.shape[1]
    ch = state_ref.shape[2]
    half = ns // 2
    opm = left_ref.shape[0]
    cz = pair_ref.shape[2]
    heads = pbw_ref.shape[0]
    wide = res * opm
    per = 128 // opm
    parts = 4
    mine = b % parts
    span = wide // parts

    first = (state_hbm, mask_hbm, left_hbm, right_hbm, pbw_hbm)
    hbm = (outer_hbm, wq_hbm, wg_hbm, pair_hbm, wk_hbm, wv_hbm, wo_hbm, up_hbm, down_hbm)
    first_to = (state_ref, mask_ref, left_ref, right_ref, pbw_ref)
    local = (outer_ref, wq_ref, wg_ref, pair_ref, wk_ref, wv_ref, wo_ref, up_ref, down_ref)
    firsts = [
        pltpu.make_async_copy(src, dst, load_sem.at[len(hbm) + k])
        for k, (src, dst) in enumerate(zip(first, first_to))
    ]
    loads = [
        pltpu.make_async_copy(src, dst, load_sem.at[k])
        for k, (src, dst) in enumerate(zip(hbm, local))
    ]

    def row_peer(t):
        c = (chip + near_to_far(t // 2) + chips) % chips
        return c * 2 + t % 2

    def col_peer(t):
        return (a + near_to_far(t) + n) % n

    for load in firsts:
        load.start()
    barrier = pltpu.get_barrier_semaphore()

    def greet(t, _):
        pl.semaphore_signal(
            barrier, inc=1, device_id={"ba": (b + t) % n}, device_id_type=pl.DeviceIdType.MESH
        )
        pl.semaphore_signal(
            barrier, inc=1, device_id={"aa": (a + t) % n}, device_id_type=pl.DeviceIdType.MESH
        )
        return 0

    lax.fori_loop(1, n, greet, 0)

    for load in loads:
        load.start()

    for load in firsts:
        load.wait()
    state = state_ref[...].reshape(ns * res, ch).astype(F32)
    normed = row_norm(state).astype(BF16)
    rows[:, b] = normed.reshape(ns, res, ch)
    for q in range(ch // 128):
        nf[q] = normed[:, q * 128 : (q + 1) * 128].astype(F32)
    by_res = jnp.concatenate(
        [
            jnp.concatenate(
                [nf[q, pl.ds(r, ns, stride=res), :] for r in range(res)], axis=0
            ).astype(BF16)
            for q in range(ch // 128)
        ],
        axis=1,
    )
    lane = lax.broadcasted_iota(jnp.int32, (opm, 128), 1)
    line = lax.broadcasted_iota(jnp.int32, (opm, 128), 0)
    rep = jnp.where(lane % opm == line, 1.0, 0.0).astype(BF16)
    lane_t = lax.broadcasted_iota(jnp.int32, (128, opm), 1)
    line_t = lax.broadcasted_iota(jnp.int32, (128, opm), 0)
    rep_t = jnp.where(line_t % opm == lane_t, 1.0, 0.0).astype(BF16)
    seg = lax.broadcasted_iota(jnp.int32, (ns, 128), 1) // opm
    keep = mask_ref[...].astype(F32).astype(BF16)
    lane_w = lax.broadcasted_iota(jnp.int32, (res, wide), 1) // opm
    line_w = lax.broadcasted_iota(jnp.int32, (res, wide), 0)
    keep_wide = mm(keep, jnp.where(lane_w == line_w, 1.0, 0.0).astype(BF16))
    keep_rep = mm(keep, rep).astype(BF16)

    def pick(parts):
        out = parts[0]
        for k in range(1, per):
            out = jnp.where(seg == k, parts[k], out)
        return out

    def factor(w_ref):
        y = mm_nt(by_res, mm(rep_t, w_ref[...]).astype(BF16))
        cols = [
            pick([y[(q * per + k) * ns : (q * per + k + 1) * ns] for k in range(per)])
            for q in range(res // per)
        ]
        return (jnp.concatenate(cols, axis=1) * keep_wide).astype(BF16)

    left = factor(left_ref)
    for k in range(parts):
        ls[k, :, :span] = left[:, k * span : (k + 1) * span]
        ls[k, :, span:] = keep_rep
    lx[b] = ls[mine]
    rz[a, :, :wide] = factor(right_ref)
    rz[a, :, wide:] = keep_rep

    pl.semaphore_wait(barrier, 2 * (n - 1))

    def to_row(buf, src, i, who, ss, rs):
        return pltpu.make_async_remote_copy(
            src_ref=src,
            dst_ref=buf,
            send_sem=ss,
            recv_sem=rs.at[i],
            device_id={"ba": who},
            device_id_type=pl.DeviceIdType.MESH,
        )

    def to_col(buf, src, i, who, ss, rs):
        return pltpu.make_async_remote_copy(
            src_ref=src,
            dst_ref=buf,
            send_sem=ss,
            recv_sem=rs.at[i],
            device_id={"aa": who},
            device_id_type=pl.DeviceIdType.MESH,
        )

    def lx_copy(i, who):
        return to_row(lx.at[i], ls.at[who % parts], i, who, lx_s, lx_r)

    def lz_copy(i, who):
        return to_col(lz.at[i, mine], lx.at[who, :, pl.ds(0, span)], i, who, lz_s, lz_r)

    def lf_copy(i, q, k, src=None):
        part = lz.at[i, q]
        return pltpu.make_async_remote_copy(
            src_ref=part if src is None else src,
            dst_ref=part,
            send_sem=lf_s,
            recv_sem=lf_r,
            device_id={"ba": b - mine + (mine + k) % parts},
            device_id_type=pl.DeviceIdType.MESH,
        )

    def ka_copy(who):
        return pltpu.make_async_remote_copy(
            src_ref=kt,
            dst_ref=ka,
            send_sem=ka_s,
            recv_sem=ka_r,
            device_id={"ba": who},
            device_id_type=pl.DeviceIdType.MESH,
        )

    def bx_copy(i, who):
        return pltpu.make_async_remote_copy(
            src_ref=tz.at[who],
            dst_ref=bx.at[i],
            send_sem=bx_s,
            recv_sem=bx_r,
            device_id={"ba": who},
            device_id_type=pl.DeviceIdType.MESH,
        )

    turn = n // 2

    def hop(buf, ss, rs, d, step, way):
        i = (a + n - way * d) % n
        part = buf.at[i]
        return pltpu.make_async_remote_copy(
            src_ref=part,
            dst_ref=part,
            send_sem=ss,
            recv_sem=rs(i, d + step, way),
            device_id={"aa": (a + n + way * step) % n},
            device_id_type=pl.DeviceIdType.MESH,
        )

    def spread(buf, ss, rs, d, reach):
        def one(step, way):
            hop(buf, ss, rs, d, step, way).start()

        for step in range(min(reach, turn - d), 0, -1):
            for way in (1, -1):
                if d + step < turn:
                    one(step, way)
                else:
                    pl.when(core == (1 - way) // 2)(functools.partial(one, step, way))

    def ring(buf, ss, rs, reach, first, last, landed):
        for d in range(first, last + 1):
            for way in (1, -1):
                if d < turn or way > 0:
                    hop(buf, ss, rs, d, 0, way).wait_recv()
            if d % reach == 0:
                spread(buf, ss, rs, d, reach)
            for way in (1, -1):
                if d < turn or way > 0:
                    landed((a + n - way * d) % n)

    def tz_at(i, d, way):
        return tz_r.at[i]

    reach = 4
    passed = [d for d in range(reach, turn, reach)]

    def rz_at(i, d, way):
        if d in passed:
            return rz_r.at[1 + 2 * passed.index(d) + (1 - way) // 2]
        return rz_r.at[0]

    def all_sent(sem, part):
        pltpu.make_async_remote_copy(
            src_ref=part,
            dst_ref=part,
            send_sem=sem,
            recv_sem=sem,
            device_id={"ba": partner},
            device_id_type=pl.DeviceIdType.MESH,
        ).wait_send()

    def all_here(sem, part):
        pltpu.make_async_remote_copy(
            src_ref=part,
            dst_ref=part,
            send_sem=sem,
            recv_sem=sem,
            device_id={"ba": partner},
            device_id_type=pl.DeviceIdType.MESH,
        ).wait_recv()

    across = chips // 2

    def x_to(i, c, step, way, d):
        part = rows.at[pl.ds(half * c, half), i]
        who = ((chip + chips + way * step) % chips) * 2 + c
        return pltpu.make_async_remote_copy(
            src_ref=part,
            dst_ref=part,
            send_sem=x_s,
            recv_sem=x1_r.at[(d + 1) // 2],
            device_id={"ba": who},
            device_id_type=pl.DeviceIdType.MESH,
        )

    def x_first():
        def one(step, way, c):
            x_to(b, c, step, way, step).start()

        for step in range(min(2, across), 0, -1):
            for way in (1, -1):
                for c in range(2):
                    if step < across:
                        one(step, way, c)
                    else:
                        pl.when(core == (1 - way) // 2)(functools.partial(one, step, way, c))

    def x_on():
        for step in range(min(2, across - 2), 0, -1):
            for way in (1, -1):
                for c in range(2):
                    if 2 + step < across or c == (1 - way) // 2:
                        i = ((chip + chips - 2 * way) % chips) * 2 + c
                        x_to(i, core, step, way, 2 + step).start()

    def x_blocks(first, last):
        return [
            ((chip + chips - way * d) % chips) * 2 + c
            for d in range(first, min(last, across) + 1)
            for way in (1, -1)
            if d < across or way > 0
            for c in range(2)
        ]

    def xf_copy(i, c, sem):
        part = rows.at[pl.ds(half * c, half), i]
        return pltpu.make_async_remote_copy(
            src_ref=part,
            dst_ref=part,
            send_sem=x_s,
            recv_sem=sem,
            device_id={"ba": partner},
            device_id_type=pl.DeviceIdType.MESH,
        )

    def start_l_off(t, _):
        lx_copy(b, row_peer(n - 1 - t)).start()
        return 0

    lx_copy(b, partner).start()
    lax.fori_loop(0, n - 2, start_l_off, 0)
    spread(rz, rz_s, rz_at, 0, reach)
    x_first()
    xf_copy(b, 1 - core, xf_r).start()
    xf_copy(b, core, xf_r).start()

    loads[0].wait()
    wf[...] = outer_ref[...].astype(F32)

    def build(d, _):
        w = wf[pl.ds(d, opm, stride=opm), :].astype(BF16)
        zero = jnp.zeros_like(w)
        for k in range(per):
            bd[pl.ds(d * 128 + k * opm, opm), :] = jnp.concatenate(
                [w if m == k else zero for m in range(per)], axis=1
            )
        return 0

    lax.fori_loop(0, opm, build, 0)

    lane_e = lax.broadcasted_iota(jnp.int32, (128, res * res), 1)
    line_e = lax.broadcasted_iota(jnp.int32, (128, res * res), 0)
    sel[...] = jnp.where(lane_e == line_e * res, 1.0, 0.0).astype(BF16)
    expand[...] = jnp.where(lane_e // res == line_e, 1.0, 0.0).astype(BF16)

    def pass_left(t, _):
        i = row_peer(t)

        @pl.when(i != b)
        def _():
            lx_copy(i, b).wait_recv()

        @pl.when(i != a)
        def _():
            lz_copy(a, i).start()

        @pl.when(i == a)
        def _():
            lz[a, mine] = lx[i, :, :span]
            for k in range(1, parts):
                lf_copy(a, mine, k, lx.at[i, :, pl.ds(0, span)]).start()

        return 0

    def nothing(i):
        pass

    lax.fori_loop(0, n * 5 // 8, pass_left, 0)
    for d in passed:
        for way in (1, -1):
            hop(rz, rz_s, rz_at, d, 0, way).wait_recv()
        spread(rz, rz_s, rz_at, d, reach)
    lax.fori_loop(n * 5 // 8, n, pass_left, 0)

    loads[1].wait()
    loads[2].wait()
    qs[...] = (mm(normed, wq_ref[...]) * ((ch // heads) ** (-0.5))).astype(BF16)
    gs[...] = jax.nn.sigmoid(mm(normed, wg_ref[...]))
    for q in range(n // per):
        vm[:, q * 128 : (q + 1) * 128] = pick(
            [lx[q * per + k, :, span:].astype(F32) for k in range(per)]
        )

    def share_left(t, _):
        i = col_peer(t)
        lz_copy(i, a).wait_recv()
        for k in range(1, parts):
            lf_copy(i, mine, k).start()
        return 0

    lax.fori_loop(1, n, share_left, 0)
    all_here(rz_r.at[0], rz.at[pl.ds(0, n - 1 - 2 * len(passed))])
    for q in range(wide // 128):
        block = rz[:, :, q * 128 : (q + 1) * 128].astype(F32).reshape(n * ns, 128)
        rt[q * 128 : (q + 1) * 128, :] = block.T
    kt[...] = rz[:, :, wide:].astype(F32).reshape(n * ns, 128).T[:res].astype(BF16)

    def send_keep(t, _):
        ka_copy((b + t) % n).start()
        return 0

    @pl.when(a == b)
    def _():
        lax.fori_loop(1, n, send_keep, 0)
        ka[...] = kt[...]

    def reorder(d, _):
        rt2[pl.ds(pl.multiple_of(d * res, res), res), :] = rt[
            pl.ds(d, res, stride=opm), :
        ].astype(BF16)
        return 0

    lax.fori_loop(0, opm, reorder, 0)


    def pass_rows(first, last, then):
        blocks = x_blocks(first, last)
        if blocks:
            many = rows.at[pl.ds(0, half), pl.ds(0, len(blocks))]
            all_here(x1_r.at[(last + 1) // 2], many)
        then()
        for i in blocks:
            xf_copy(i, core, xf_r).start()

    pass_rows(1, 2, x_on)
    all_here(lf_r, lz.at[:, pl.ds(0, parts - 1)])

    groups = res // per
    for g in range(groups // 2):
        at = g * 256 % span
        block = lz[:, g * 256 // span, :, at : at + 256].astype(F32)
        lb[g] = block.reshape(n * ns, 256).astype(BF16)

    def outer(g, _):
        block = mm(rt2[...], lb[g]).astype(BF16)
        for k in range(2):
            at = pl.ds(pl.multiple_of((2 * g + k) * res, res), res)
            for d in range(opm):
                lhs[at, d * 128 : (d + 1) * 128] = block[
                    d * res : (d + 1) * res, k * 128 : (k + 1) * 128
                ]
        return 0

    lax.fori_loop(0, groups // 2, outer, 0)
    upd[...] = mm(lhs[...], bd[...])


    @pl.when(a != b)
    def _():
        ka_copy(a).wait_recv()

    inverse = 1.0 / mm_nt(kt[...], ka[...])
    loads[3].wait()
    step = 8
    for at in range(0, res, step):
        block = jnp.concatenate(
            [
                upd[i // per * res : (i // per + 1) * res, i % per * 128 : (i % per + 1) * 128]
                * inverse[:, i : i + 1]
                for i in range(at, at + step)
            ],
            axis=0,
        )
        old = pair_ref[at : at + step].reshape(step * res, cz).astype(F32)
        fresh = (old + block).astype(BF16)
        pair_out[at : at + step] = fresh.reshape(step, res, cz)
        pn[at * res : (at + step) * res, :] = row_norm(fresh.astype(F32)).astype(BF16)
    tile = mm_nt(pbw_ref[...], pn[...])
    lane_t = lax.broadcasted_iota(jnp.int32, (heads, 128), 1)
    base = []
    for v in range(res // per):
        top = tile[:, v * 128 : (v + 1) * 128]
        by = 1
        while by < res:
            other = jnp.where(
                lane_t // by % 2 == 1, pltpu.roll(top, by, 1), pltpu.roll(top, 128 - by, 1)
            )
            top = jnp.maximum(top, other)
            by *= 2
        base.append(top)
    base = jnp.concatenate(base, axis=1).astype(BF16)
    tz[a, :, : res * res] = (tile - base.astype(F32)).astype(BF16)
    tz[a, :, res * res :] = mm_nt(base, sel[...]).astype(BF16)
    spread(tz, tz_s, tz_at, 0, 4)
    store = pltpu.make_async_copy(pair_out, pair_hbm_out, store_sem.at[0])
    store.start()

    pass_rows(3, 4, lambda: None)
    def pass_bias(i):
        @pl.when(i != b)
        def _():
            bx_copy(b, i).start()

        @pl.when(i == b)
        def _():
            bx[b] = tz[i]

    pass_bias(a)
    ring(tz, tz_s, tz_at, 4, 1, min(4, turn), pass_bias)
    all_here(xf_r, rows.at[pl.ds(0, half), pl.ds(0, n)])
    head_lane = lax.broadcasted_iota(jnp.int32, (res, ch), 1) // (ch // heads)

    loads[4].wait()
    loads[5].wait()

    def score(s, _):
        x = rows[s].reshape(n * res, ch)
        key = mm(x, wk_ref[...]).astype(BF16)
        kv[s] = mm(x, wv_ref[...]).astype(BF16)
        q = qs[pl.ds(pl.multiple_of(s * res, res), res), :].astype(F32)
        query = jnp.concatenate(
            [jnp.where(head_lane == h, q, 0.0) for h in range(heads)], axis=0
        ).astype(BF16)
        sc[s] = mm_nt(query, key)
        return 0

    lax.fori_loop(0, ns, score, 0, unroll=2)
    ring(tz, tz_s, tz_at, 4, 5, turn, pass_bias)

    others = pl.ds(0, n - 1)
    all_sent(lx_s, lx.at[others])
    all_sent(lz_s, lz.at[others, 0])
    all_sent(lf_s, lz.at[:, pl.ds(0, parts - 1)])
    all_sent(rz_s, rz.at[others])
    all_sent(x_s, rows.at[:, others])

    @pl.when(a == b)
    def _():
        all_sent(ka_s, pn.at[pl.ds(0, (n - 1) * res)])

    store.wait()
    for load in loads[6:]:
        load.wait()

    all_here(bx_r, bx.at[others])
    base = bx[:, :, res * res :].astype(F32).reshape(n * heads, 128).astype(BF16)
    base = mm(base, expand[...])
    for q in range(n // per):
        for v in range(res // per):
            cols = slice(v * 128, (v + 1) * 128)
            cut = [
                bx[q * per + k, :, cols].astype(F32)
                + base[(q * per + k) * heads : (q * per + k + 1) * heads, cols]
                for k in range(per)
            ]
            turned = [cut[0]] + [pltpu.roll(cut[k], opm * k, 1) for k in range(1, per)]
            for m in range(per):
                mixed = pick([turned[(k - m) % per] for k in range(per)])
                if m:
                    mixed = pltpu.roll(mixed, 128 - opm * m, 1)
                i = v * per + m
                bi[q, i * heads : (i + 1) * heads, :] = mixed
        for h in range(heads):
            bh[h * res : (h + 1) * res, q * 128 : (q + 1) * 128] = bi[
                q, pl.ds(h, res, stride=heads), :
            ]

    def attend(s, _):
        valid = vm[pl.ds(s, 1), :]
        scores = jnp.where(valid > 0, sc[s] + bh[...], -1000000000.0)
        top = jnp.max(scores, axis=-1, keepdims=True)
        raw = jnp.exp(scores - top)
        mass = jnp.sum(raw, axis=-1, keepdims=True)
        mixed = mm(raw.astype(BF16), kv[s]) / mass
        out = mixed[:res]
        for h in range(1, heads):
            out = jnp.where(head_lane == h, mixed[h * res : (h + 1) * res], out)
        at = pl.ds(pl.multiple_of(s * res, res), res)
        gated[at, :] = (out * gs[at, :]).astype(BF16)
        return 0

    lax.fori_loop(0, ns, attend, 0, unroll=4)

    middle = state_ref[...].reshape(ns * res, ch).astype(F32) + mm(gated[...], wo_ref[...])
    hidden = jnp.maximum(mm(row_norm(middle).astype(BF16), up_ref[...]), 0.0).astype(BF16)
    final = middle + mm(hidden, down_ref[...])
    msa_out[...] = final.astype(BF16).reshape(ns, res, ch)
    store = pltpu.make_async_copy(msa_out, msa_hbm_out, store_sem.at[1])
    store.start()
    all_sent(tz_s, tz.at[others])
    all_sent(bx_s, bx.at[others])
    store.wait()


def per_device(n, *args):
    state, pair, mask, left, _, _, pbw = args[:7]
    ns, res, ch = state.shape
    opm, heads, cz = left.shape[1], pbw.shape[1], pair.shape[2]
    args = args[:3] + (left.T, args[4].T, args[5], pbw.T) + args[7:]
    wide = res * opm
    parts = 4
    span = wide // parts
    per = 128 // opm
    groups = res // per
    keys = n * res
    dma = pltpu.SemaphoreType.DMA((n,))
    vmem = pl.BlockSpec(memory_space=pltpu.VMEM)
    far = pl.BlockSpec(memory_space=pl.ANY)
    order = (0, 2, 3, 4, 6, 1, 5, 7, 8, 9, 10, 11, 12, 13)
    return tuple(
        pl.pallas_call(
            functools.partial(body, n),
            out_shape=(
                jax.ShapeDtypeStruct(state.shape, BF16),
                jax.ShapeDtypeStruct(pair.shape, BF16),
            ),
            in_specs=[far] * len(args),
            out_specs=(far, far),
            scratch_shapes=[pltpu.VMEM(args[k].shape, args[k].dtype) for k in order]
            + [
                pltpu.VMEM(pair.shape, BF16),
                pltpu.VMEM(state.shape, BF16),
                pltpu.SemaphoreType.DMA((len(order),)),
                pltpu.SemaphoreType.DMA((2,)),
                pltpu.VMEM((ns, n, res, ch), BF16),
                pltpu.VMEM((ch // 128, ns * res, 128), F32),
                pltpu.VMEM((parts, ns, span + 128), BF16),
                pltpu.VMEM((n, ns, span + 128), BF16),
                pltpu.VMEM((n, parts, ns, span), BF16),
                pltpu.VMEM((n, ns, wide + 128), BF16),
                pltpu.VMEM((n, heads, res * res + 128), BF16),
                pltpu.VMEM((n, heads, res * res + 128), BF16),
                pltpu.VMEM((res, n * ns), BF16),
                pltpu.VMEM((res, n * ns), BF16),
                pltpu.VMEM((128, res * res), BF16),
                pltpu.VMEM((128, res * res), BF16),
                pltpu.VMEM((wide, n * ns), F32),
                pltpu.VMEM((wide, n * ns), BF16),
                pltpu.VMEM((groups // 2, n * ns, 256), BF16),
                pltpu.VMEM((opm * opm, cz), F32),
                pltpu.VMEM((opm * 128, per * cz), BF16),
                pltpu.VMEM((groups * res, opm * 128), BF16),
                pltpu.VMEM((groups * res, per * cz), F32),
                pltpu.VMEM((res * res, cz), BF16),
                pltpu.VMEM((keys // 128, res * heads, 128), F32),
                pltpu.VMEM((heads * res, keys), F32),
                pltpu.VMEM((ns, keys, ch), BF16),
                pltpu.VMEM((ns, heads * res, keys), F32),
                pltpu.VMEM((ns * res, ch), BF16),
                pltpu.VMEM((ns * res, ch), F32),
                pltpu.VMEM((ns, keys), F32),
                pltpu.VMEM((ns * res, ch), BF16),
            ]
            + [pltpu.SemaphoreType.DMA] * 8
            + [dma] * 3
            + [pltpu.SemaphoreType.DMA((3,))] * 2
            + [pltpu.SemaphoreType.DMA] * 4,
            compiler_params=pltpu.CompilerParams(
                collective_id=0, has_side_effects=True, vmem_limit_bytes=52 * 1024 * 1024
            ),
        )(*[pltpu.with_memory_space_constraint(x, pltpu.HBM) for x in args])
    )


def solution(mesh):
    spec = P(("groups", "aa"), "ba", None)
    return jax.shard_map(
        functools.partial(per_device, mesh.shape["ba"]),
        mesh=mesh,
        in_specs=(spec, spec, P(("groups", "aa"), "ba")) + (P(),) * 11,
        out_specs=(spec, spec),
        check_vma=False,
    )
```

```python
import functools

import jax
import jax.numpy as jnp
from jax import lax
from jax.experimental import pallas as pl
from jax.experimental.pallas import tpu as pltpu
from jax.sharding import PartitionSpec as P

F32 = jnp.float32
BF16 = jnp.bfloat16
NT = (((1,), (1,)), ((), ()))


def mm(x, y):
    return jnp.dot(x, y, preferred_element_type=F32)


def mm_nt(x, y):
    return lax.dot_general(x, y, NT, preferred_element_type=F32)


def row_norm(values):
    center = values - jnp.mean(values, axis=-1, keepdims=True)
    spread = jnp.mean(center * center, axis=-1, keepdims=True)
    return center * lax.rsqrt(spread + 1e-05)


def near_to_far(t):
    return ((t + 1) // 2) * (2 * (t % 2) - 1)


def body(
    n,
    state_hbm,
    pair_hbm,
    mask_hbm,
    left_hbm,
    right_hbm,
    outer_hbm,
    pbw_hbm,
    wq_hbm,
    wk_hbm,
    wv_hbm,
    wg_hbm,
    wo_hbm,
    up_hbm,
    down_hbm,
    msa_hbm_out,
    pair_hbm_out,
    state_ref,
    mask_ref,
    left_ref,
    right_ref,
    pbw_ref,
    pair_ref,
    outer_ref,
    wq_ref,
    wk_ref,
    wv_ref,
    wg_ref,
    wo_ref,
    up_ref,
    down_ref,
    pair_out,
    msa_out,
    load_sem,
    store_sem,
    rows,
    nf,
    ls,
    lx,
    lz,
    rz,
    tz,
    bx,
    kt,
    ka,
    sel,
    expand,
    rt,
    rt2,
    wf,
    bd,
    lhs,
    upd,
    pn,
    bi,
    bh,
    kv,
    sc,
    qs,
    gs,
    vm,
    lx_s,
    lz_s,
    lf_s,
    ka_s,
    rz_s,
    x_s,
    tz_s,
    bx_s,
    lx_r,
    lz_r,
    tz_r,
    rz_r,
    x1_r,
    bx_r,
    lf_r,
    ka_r,
    xf_r,
):
    a = lax.axis_index("aa")
    b = lax.axis_index("ba")
    core = b % 2
    chip = b // 2
    chips = n // 2
    partner = chip * 2 + 1 - core
    ns = state_ref.shape[0]
    res = state_ref.shape[1]
    ch = state_ref.shape[2]
    half = ns // 2
    opm = left_ref.shape[0]
    cz = pair_ref.shape[2]
    heads = pbw_ref.shape[0]
    wide = res * opm
    per = 128 // opm
    parts = 4
    mine = b % parts
    span = wide // parts

    first = (state_hbm, mask_hbm, left_hbm, right_hbm, pbw_hbm)
    hbm = (outer_hbm, wq_hbm, wg_hbm, pair_hbm, wk_hbm, wv_hbm, wo_hbm, up_hbm, down_hbm)
    first_to = (state_ref, mask_ref, left_ref, right_ref, pbw_ref)
    local = (outer_ref, wq_ref, wg_ref, pair_ref, wk_ref, wv_ref, wo_ref, up_ref, down_ref)
    firsts = [
        pltpu.make_async_copy(src, dst, load_sem.at[len(hbm) + k])
        for k, (src, dst) in enumerate(zip(first, first_to))
    ]
    loads = [
        pltpu.make_async_copy(src, dst, load_sem.at[k])
        for k, (src, dst) in enumerate(zip(hbm, local))
    ]

    def row_peer(t):
        c = (chip + near_to_far(t // 2) + chips) % chips
        return c * 2 + t % 2

    def col_peer(t):
        return (a + near_to_far(t) + n) % n

    for load in firsts:
        load.start()
    barrier = pltpu.get_barrier_semaphore()

    def greet(t, _):
        pl.semaphore_signal(
            barrier, inc=1, device_id={"ba": (b + t) % n}, device_id_type=pl.DeviceIdType.MESH
        )
        pl.semaphore_signal(
            barrier, inc=1, device_id={"aa": (a + t) % n}, device_id_type=pl.DeviceIdType.MESH
        )
        return 0

    lax.fori_loop(1, n, greet, 0)

    for load in loads:
        load.start()

    for load in firsts:
        load.wait()
    state = state_ref[...].reshape(ns * res, ch).astype(F32)
    normed = row_norm(state).astype(BF16)
    rows[:, b] = normed.reshape(ns, res, ch)
    for q in range(ch // 128):
        nf[q] = normed[:, q * 128 : (q + 1) * 128].astype(F32)
    by_res = jnp.concatenate(
        [
            jnp.concatenate(
                [nf[q, pl.ds(r, ns, stride=res), :] for r in range(res)], axis=0
            ).astype(BF16)
            for q in range(ch // 128)
        ],
        axis=1,
    )
    lane = lax.broadcasted_iota(jnp.int32, (opm, 128), 1)
    line = lax.broadcasted_iota(jnp.int32, (opm, 128), 0)
    rep = jnp.where(lane % opm == line, 1.0, 0.0).astype(BF16)
    lane_t = lax.broadcasted_iota(jnp.int32, (128, opm), 1)
    line_t = lax.broadcasted_iota(jnp.int32, (128, opm), 0)
    rep_t = jnp.where(line_t % opm == lane_t, 1.0, 0.0).astype(BF16)
    seg = lax.broadcasted_iota(jnp.int32, (ns, 128), 1) // opm
    keep = mask_ref[...].astype(F32).astype(BF16)
    lane_w = lax.broadcasted_iota(jnp.int32, (res, wide), 1) // opm
    line_w = lax.broadcasted_iota(jnp.int32, (res, wide), 0)
    keep_wide = mm(keep, jnp.where(lane_w == line_w, 1.0, 0.0).astype(BF16))
    keep_rep = mm(keep, rep).astype(BF16)

    def pick(parts):
        out = parts[0]
        for k in range(1, per):
            out = jnp.where(seg == k, parts[k], out)
        return out

    def factor(w_ref):
        y = mm_nt(by_res, mm(rep_t, w_ref[...]).astype(BF16))
        cols = [
            pick([y[(q * per + k) * ns : (q * per + k + 1) * ns] for k in range(per)])
            for q in range(res // per)
        ]
        return (jnp.concatenate(cols, axis=1) * keep_wide).astype(BF16)

    left = factor(left_ref)
    for k in range(parts):
        ls[k, :, :span] = left[:, k * span : (k + 1) * span]
        ls[k, :, span:] = keep_rep
    lx[b] = ls[mine]
    rz[a, :, :wide] = factor(right_ref)
    rz[a, :, wide:] = keep_rep

    pl.semaphore_wait(barrier, 2 * (n - 1))

    def to_row(buf, src, i, who, ss, rs):
        return pltpu.make_async_remote_copy(
            src_ref=src,
            dst_ref=buf,
            send_sem=ss,
            recv_sem=rs.at[i],
            device_id={"ba": who},
            device_id_type=pl.DeviceIdType.MESH,
        )

    def to_col(buf, src, i, who, ss, rs):
        return pltpu.make_async_remote_copy(
            src_ref=src,
            dst_ref=buf,
            send_sem=ss,
            recv_sem=rs.at[i],
            device_id={"aa": who},
            device_id_type=pl.DeviceIdType.MESH,
        )

    def lx_copy(i, who):
        return to_row(lx.at[i], ls.at[who % parts], i, who, lx_s, lx_r)

    def lz_copy(i, who):
        return to_col(lz.at[i, mine], lx.at[who, :, pl.ds(0, span)], i, who, lz_s, lz_r)

    def lf_copy(i, q, k, src=None):
        part = lz.at[i, q]
        return pltpu.make_async_remote_copy(
            src_ref=part if src is None else src,
            dst_ref=part,
            send_sem=lf_s,
            recv_sem=lf_r,
            device_id={"ba": b - mine + (mine + k) % parts},
            device_id_type=pl.DeviceIdType.MESH,
        )

    def ka_copy(who):
        return pltpu.make_async_remote_copy(
            src_ref=kt,
            dst_ref=ka,
            send_sem=ka_s,
            recv_sem=ka_r,
            device_id={"ba": who},
            device_id_type=pl.DeviceIdType.MESH,
        )

    def bx_copy(i, who):
        return pltpu.make_async_remote_copy(
            src_ref=tz.at[who],
            dst_ref=bx.at[i],
            send_sem=bx_s,
            recv_sem=bx_r,
            device_id={"ba": who},
            device_id_type=pl.DeviceIdType.MESH,
        )

    turn = n // 2

    def hop(buf, ss, rs, d, step, way):
        i = (a + n - way * d) % n
        part = buf.at[i]
        return pltpu.make_async_remote_copy(
            src_ref=part,
            dst_ref=part,
            send_sem=ss,
            recv_sem=rs(i, d + step, way),
            device_id={"aa": (a + n + way * step) % n},
            device_id_type=pl.DeviceIdType.MESH,
        )

    def spread(buf, ss, rs, d, reach):
        def one(step, way):
            hop(buf, ss, rs, d, step, way).start()

        for step in range(min(reach, turn - d), 0, -1):
            for way in (1, -1):
                if d + step < turn:
                    one(step, way)
                else:
                    pl.when(core == (1 - way) // 2)(functools.partial(one, step, way))

    def ring(buf, ss, rs, reach, first, last, landed):
        for d in range(first, last + 1):
            for way in (1, -1):
                if d < turn or way > 0:
                    hop(buf, ss, rs, d, 0, way).wait_recv()
            if d % reach == 0:
                spread(buf, ss, rs, d, reach)
            for way in (1, -1):
                if d < turn or way > 0:
                    landed((a + n - way * d) % n)

    def tz_at(i, d, way):
        return tz_r.at[i]

    reach = 4
    passed = [d for d in range(reach, turn, reach)]

    def rz_at(i, d, way):
        if d in passed:
            return rz_r.at[1 + 2 * passed.index(d) + (1 - way) // 2]
        return rz_r.at[0]

    def all_sent(sem, part):
        pltpu.make_async_remote_copy(
            src_ref=part,
            dst_ref=part,
            send_sem=sem,
            recv_sem=sem,
            device_id={"ba": partner},
            device_id_type=pl.DeviceIdType.MESH,
        ).wait_send()

    def all_here(sem, part):
        pltpu.make_async_remote_copy(
            src_ref=part,
            dst_ref=part,
            send_sem=sem,
            recv_sem=sem,
            device_id={"ba": partner},
            device_id_type=pl.DeviceIdType.MESH,
        ).wait_recv()

    across = chips // 2

    def x_to(i, c, step, way, d):
        part = rows.at[pl.ds(half * c, half), i]
        who = ((chip + chips + way * step) % chips) * 2 + c
        return pltpu.make_async_remote_copy(
            src_ref=part,
            dst_ref=part,
            send_sem=x_s,
            recv_sem=x1_r.at[(d + 1) // 2],
            device_id={"ba": who},
            device_id_type=pl.DeviceIdType.MESH,
        )

    def x_first():
        def one(step, way, c):
            x_to(b, c, step, way, step).start()

        for step in range(min(2, across), 0, -1):
            for way in (1, -1):
                for c in range(2):
                    if step < across:
                        one(step, way, c)
                    else:
                        pl.when(core == (1 - way) // 2)(functools.partial(one, step, way, c))

    def x_on():
        for step in range(min(2, across - 2), 0, -1):
            for way in (1, -1):
                for c in range(2):
                    if 2 + step < across or c == (1 - way) // 2:
                        i = ((chip + chips - 2 * way) % chips) * 2 + c
                        x_to(i, core, step, way, 2 + step).start()

    def x_blocks(first, last):
        return [
            ((chip + chips - way * d) % chips) * 2 + c
            for d in range(first, min(last, across) + 1)
            for way in (1, -1)
            if d < across or way > 0
            for c in range(2)
        ]

    def xf_copy(i, c, sem):
        part = rows.at[pl.ds(half * c, half), i]
        return pltpu.make_async_remote_copy(
            src_ref=part,
            dst_ref=part,
            send_sem=x_s,
            recv_sem=sem,
            device_id={"ba": partner},
            device_id_type=pl.DeviceIdType.MESH,
        )

    def start_l_off(t, _):
        lx_copy(b, row_peer(n - 1 - t)).start()
        return 0

    lx_copy(b, partner).start()
    lax.fori_loop(0, n - 2, start_l_off, 0)
    spread(rz, rz_s, rz_at, 0, reach)
    x_first()
    xf_copy(b, 1 - core, xf_r).start()
    xf_copy(b, core, xf_r).start()

    loads[0].wait()
    wf[...] = outer_ref[...].astype(F32)

    def build(d, _):
        w = wf[pl.ds(d, opm, stride=opm), :].astype(BF16)
        zero = jnp.zeros_like(w)
        for k in range(per):
            bd[pl.ds(d * 128 + k * opm, opm), :] = jnp.concatenate(
                [w if m == k else zero for m in range(per)], axis=1
            )
        return 0

    lax.fori_loop(0, opm, build, 0)

    lane_e = lax.broadcasted_iota(jnp.int32, (128, res * res), 1)
    line_e = lax.broadcasted_iota(jnp.int32, (128, res * res), 0)
    sel[...] = jnp.where(lane_e == line_e * res, 1.0, 0.0).astype(BF16)
    expand[...] = jnp.where(lane_e // res == line_e, 1.0, 0.0).astype(BF16)

    def pass_left(t, _):
        i = row_peer(t)

        @pl.when(i != b)
        def _():
            lx_copy(i, b).wait_recv()

        @pl.when(i != a)
        def _():
            lz_copy(a, i).start()

        @pl.when(i == a)
        def _():
            lz[a, mine] = lx[i, :, :span]
            for k in range(1, parts):
                lf_copy(a, mine, k, lx.at[i, :, pl.ds(0, span)]).start()

        return 0

    def nothing(i):
        pass

    lax.fori_loop(0, n * 5 // 8, pass_left, 0)
    lax.fori_loop(n * 5 // 8, n, pass_left, 0)

    for d in passed:
        for way in (1, -1):
            hop(rz, rz_s, rz_at, d, 0, way).wait_recv()
        spread(rz, rz_s, rz_at, d, reach)

    loads[1].wait()
    loads[2].wait()
    qs[...] = (mm(normed, wq_ref[...]) * ((ch // heads) ** (-0.5))).astype(BF16)
    gs[...] = jax.nn.sigmoid(mm(normed, wg_ref[...]))
    for q in range(n // per):
        vm[:, q * 128 : (q + 1) * 128] = pick(
            [lx[q * per + k, :, span:].astype(F32) for k in range(per)]
        )

    def share_left(t, _):
        i = col_peer(t)
        lz_copy(i, a).wait_recv()
        for k in range(1, parts):
            lf_copy(i, mine, k).start()
        return 0

    lax.fori_loop(1, n, share_left, 0)
    all_here(rz_r.at[0], rz.at[pl.ds(0, n - 1 - 2 * len(passed))])
    kt[...] = rz[:, :, wide:].astype(F32).reshape(n * ns, 128).T[:res].astype(BF16)

    def send_keep(t, _):
        ka_copy((b + t) % n).start()
        return 0

    @pl.when(a == b)
    def _():
        lax.fori_loop(1, n, send_keep, 0)
        ka[...] = kt[...]

    for q in range(wide // 128):
        block = rz[:, :, q * 128 : (q + 1) * 128].astype(F32).reshape(n * ns, 128)
        rt[q * 128 : (q + 1) * 128, :] = block.T

    def reorder(d, _):
        rt2[pl.ds(pl.multiple_of(d * res, res), res), :] = rt[
            pl.ds(d, res, stride=opm), :
        ].astype(BF16)
        return 0

    lax.fori_loop(0, opm, reorder, 0)


    def pass_rows(first, last, then):
        blocks = x_blocks(first, last)
        if blocks:
            many = rows.at[pl.ds(0, half), pl.ds(0, len(blocks))]
            all_here(x1_r.at[(last + 1) // 2], many)
        then()
        for i in blocks:
            xf_copy(i, core, xf_r).start()

    pass_rows(1, 2, x_on)
    def outer(k, _):
        g = (mine + k) % parts
        left = lz[:, g].astype(F32).reshape(n * ns, span).astype(BF16)
        block = mm(rt2[...], left).astype(BF16)
        for k in range(span // 128):
            at = pl.ds(pl.multiple_of((span // 128 * g + k) * res, res), res)
            for d in range(opm):
                lhs[at, d * 128 : (d + 1) * 128] = block[
                    d * res : (d + 1) * res, k * 128 : (k + 1) * 128
                ]
        return 0

    outer(0, 0)
    all_here(lf_r, lz.at[:, pl.ds(0, parts - 1)])
    lax.fori_loop(1, parts, outer, 0)
    upd[...] = mm(lhs[...], bd[...])


    @pl.when(a != b)
    def _():
        ka_copy(a).wait_recv()

    inverse = 1.0 / mm_nt(kt[...], ka[...])
    loads[3].wait()
    step = 8
    for at in range(0, res, step):
        block = jnp.concatenate(
            [
                upd[i // per * res : (i // per + 1) * res, i % per * 128 : (i % per + 1) * 128]
                * inverse[:, i : i + 1]
                for i in range(at, at + step)
            ],
            axis=0,
        )
        old = pair_ref[at : at + step].reshape(step * res, cz).astype(F32)
        fresh = (old + block).astype(BF16)
        pair_out[at : at + step] = fresh.reshape(step, res, cz)
        pn[at * res : (at + step) * res, :] = row_norm(fresh.astype(F32)).astype(BF16)
    tile = mm_nt(pbw_ref[...], pn[...])
    lane_t = lax.broadcasted_iota(jnp.int32, (heads, 128), 1)
    base = []
    for v in range(res // per):
        top = tile[:, v * 128 : (v + 1) * 128]
        by = 1
        while by < res:
            other = jnp.where(
                lane_t // by % 2 == 1, pltpu.roll(top, by, 1), pltpu.roll(top, 128 - by, 1)
            )
            top = jnp.maximum(top, other)
            by *= 2
        base.append(top)
    base = jnp.concatenate(base, axis=1).astype(BF16)
    tz[a, :, : res * res] = (tile - base.astype(F32)).astype(BF16)
    tz[a, :, res * res :] = mm_nt(base, sel[...]).astype(BF16)
    spread(tz, tz_s, tz_at, 0, 4)
    store = pltpu.make_async_copy(pair_out, pair_hbm_out, store_sem.at[0])
    store.start()

    pass_rows(3, 4, lambda: None)
    def pass_bias(i):
        @pl.when(i != b)
        def _():
            bx_copy(b, i).start()

        @pl.when(i == b)
        def _():
            bx[b] = tz[i]

    pass_bias(a)
    ring(tz, tz_s, tz_at, 4, 1, min(4, turn), pass_bias)
    all_here(xf_r, rows.at[pl.ds(0, half), pl.ds(0, n)])
    head_lane = lax.broadcasted_iota(jnp.int32, (res, ch), 1) // (ch // heads)

    loads[4].wait()
    loads[5].wait()

    def score(s, _):
        x = rows[s].reshape(n * res, ch)
        key = mm(x, wk_ref[...]).astype(BF16)
        kv[s] = mm(x, wv_ref[...]).astype(BF16)
        q = qs[pl.ds(pl.multiple_of(s * res, res), res), :].astype(F32)
        query = jnp.concatenate(
            [jnp.where(head_lane == h, q, 0.0) for h in range(heads)], axis=0
        ).astype(BF16)
        sc[s] = mm_nt(query, key)
        return 0

    lax.fori_loop(0, ns, score, 0, unroll=2)
    ring(tz, tz_s, tz_at, 4, 5, turn, pass_bias)

    others = pl.ds(0, n - 1)
    all_sent(lx_s, lx.at[others])
    all_sent(lz_s, lz.at[others, 0])
    all_sent(lf_s, lz.at[:, pl.ds(0, parts - 1)])
    all_sent(rz_s, rz.at[others])
    all_sent(x_s, rows.at[:, others])

    @pl.when(a == b)
    def _():
        all_sent(ka_s, pn.at[pl.ds(0, (n - 1) * res)])

    store.wait()
    for load in loads[6:]:
        load.wait()

    all_here(bx_r, bx.at[others])
    base = bx[:, :, res * res :].astype(F32).reshape(n * heads, 128).astype(BF16)
    base = mm(base, expand[...])
    for q in range(n // per):
        for v in range(res // per):
            cols = slice(v * 128, (v + 1) * 128)
            cut = [
                bx[q * per + k, :, cols].astype(F32)
                + base[(q * per + k) * heads : (q * per + k + 1) * heads, cols]
                for k in range(per)
            ]
            turned = [cut[0]] + [pltpu.roll(cut[k], opm * k, 1) for k in range(1, per)]
            for m in range(per):
                mixed = pick([turned[(k - m) % per] for k in range(per)])
                if m:
                    mixed = pltpu.roll(mixed, 128 - opm * m, 1)
                i = v * per + m
                bi[q, i * heads : (i + 1) * heads, :] = mixed
        for h in range(heads):
            bh[h * res : (h + 1) * res, q * 128 : (q + 1) * 128] = bi[
                q, pl.ds(h, res, stride=heads), :
            ]

    def attend(s):
        scores = jnp.where(vm[s : s + 1, :] > 0, sc[s] + bh[...], -1000000000.0)
        top = jnp.max(scores, axis=-1, keepdims=True)
        raw = jnp.exp(scores - top)
        mass = jnp.sum(raw, axis=-1, keepdims=True)
        mixed = mm(raw.astype(BF16), kv[s]) / mass
        out = mixed[:res]
        for h in range(1, heads):
            out = jnp.where(head_lane == h, mixed[h * res : (h + 1) * res], out)
        return (out * gs[s * res : (s + 1) * res, :]).astype(BF16)

    stores = []
    for k in range(2):
        these = slice(k * half, (k + 1) * half)
        gated = jnp.concatenate([attend(s) for s in range(k * half, (k + 1) * half)], axis=0)
        middle = state_ref[these].reshape(half * res, ch).astype(F32) + mm(gated, wo_ref[...])
        hidden = jnp.maximum(mm(row_norm(middle).astype(BF16), up_ref[...]), 0.0).astype(BF16)
        final = middle + mm(hidden, down_ref[...])
        msa_out[these] = final.astype(BF16).reshape(half, res, ch)
        at = pl.ds(k * half, half)
        stores.append(
            pltpu.make_async_copy(msa_out.at[at], msa_hbm_out.at[at], store_sem.at[1 + k])
        )
        stores[k].start()
    all_sent(tz_s, tz.at[others])
    all_sent(bx_s, bx.at[others])
    for store in stores:
        store.wait()


def per_device(n, *args):
    state, pair, mask, left, _, _, pbw = args[:7]
    ns, res, ch = state.shape
    opm, heads, cz = left.shape[1], pbw.shape[1], pair.shape[2]
    args = args[:3] + (left.T, args[4].T, args[5], pbw.T) + args[7:]
    wide = res * opm
    parts = 4
    span = wide // parts
    per = 128 // opm
    groups = res // per
    keys = n * res
    dma = pltpu.SemaphoreType.DMA((n,))
    vmem = pl.BlockSpec(memory_space=pltpu.VMEM)
    far = pl.BlockSpec(memory_space=pl.ANY)
    order = (0, 2, 3, 4, 6, 1, 5, 7, 8, 9, 10, 11, 12, 13)
    return tuple(
        pl.pallas_call(
            functools.partial(body, n),
            out_shape=(
                jax.ShapeDtypeStruct(state.shape, BF16),
                jax.ShapeDtypeStruct(pair.shape, BF16),
            ),
            in_specs=[far] * len(args),
            out_specs=(far, far),
            scratch_shapes=[pltpu.VMEM(args[k].shape, args[k].dtype) for k in order]
            + [
                pltpu.VMEM(pair.shape, BF16),
                pltpu.VMEM(state.shape, BF16),
                pltpu.SemaphoreType.DMA((len(order),)),
                pltpu.SemaphoreType.DMA((3,)),
                pltpu.VMEM((ns, n, res, ch), BF16),
                pltpu.VMEM((ch // 128, ns * res, 128), F32),
                pltpu.VMEM((parts, ns, span + 128), BF16),
                pltpu.VMEM((n, ns, span + 128), BF16),
                pltpu.VMEM((n, parts, ns, span), BF16),
                pltpu.VMEM((n, ns, wide + 128), BF16),
                pltpu.VMEM((n, heads, res * res + 128), BF16),
                pltpu.VMEM((n, heads, res * res + 128), BF16),
                pltpu.VMEM((res, n * ns), BF16),
                pltpu.VMEM((res, n * ns), BF16),
                pltpu.VMEM((128, res * res), BF16),
                pltpu.VMEM((128, res * res), BF16),
                pltpu.VMEM((wide, n * ns), F32),
                pltpu.VMEM((wide, n * ns), BF16),
                pltpu.VMEM((opm * opm, cz), F32),
                pltpu.VMEM((opm * 128, per * cz), BF16),
                pltpu.VMEM((groups * res, opm * 128), BF16),
                pltpu.VMEM((groups * res, per * cz), F32),
                pltpu.VMEM((res * res, cz), BF16),
                pltpu.VMEM((keys // 128, res * heads, 128), F32),
                pltpu.VMEM((heads * res, keys), F32),
                pltpu.VMEM((ns, keys, ch), BF16),
                pltpu.VMEM((ns, heads * res, keys), F32),
                pltpu.VMEM((ns * res, ch), BF16),
                pltpu.VMEM((ns * res, ch), F32),
                pltpu.VMEM((ns, keys), F32),
            ]
            + [pltpu.SemaphoreType.DMA] * 8
            + [dma] * 3
            + [pltpu.SemaphoreType.DMA((3,))] * 2
            + [pltpu.SemaphoreType.DMA] * 4,
            compiler_params=pltpu.CompilerParams(
                collective_id=0, has_side_effects=True, vmem_limit_bytes=52 * 1024 * 1024
            ),
        )(*[pltpu.with_memory_space_constraint(x, pltpu.HBM) for x in args])
    )


def solution(mesh):
    spec = P(("groups", "aa"), "ba", None)
    return jax.shard_map(
        functools.partial(per_device, mesh.shape["ba"]),
        mesh=mesh,
        in_specs=(spec, spec, P(("groups", "aa"), "ba")) + (P(),) * 11,
        out_specs=(spec, spec),
        check_vma=False,
    )
```

```python
import functools

import jax
import jax.numpy as jnp
from jax import lax
from jax.experimental import pallas as pl
from jax.experimental.pallas import tpu as pltpu
from jax.sharding import PartitionSpec as P

F32 = jnp.float32
BF16 = jnp.bfloat16
NT = (((1,), (1,)), ((), ()))


def mm(x, y):
    return jnp.dot(x, y, preferred_element_type=F32)


def mm_nt(x, y):
    return lax.dot_general(x, y, NT, preferred_element_type=F32)


def row_norm(values):
    center = values - jnp.mean(values, axis=-1, keepdims=True)
    spread = jnp.mean(center * center, axis=-1, keepdims=True)
    return center * lax.rsqrt(spread + 1e-05)


def near_to_far(t):
    return ((t + 1) // 2) * (2 * (t % 2) - 1)


def body(
    n,
    state_hbm,
    pair_hbm,
    mask_hbm,
    left_hbm,
    right_hbm,
    outer_hbm,
    pbw_hbm,
    wq_hbm,
    wk_hbm,
    wv_hbm,
    wg_hbm,
    wo_hbm,
    up_hbm,
    down_hbm,
    msa_hbm_out,
    pair_hbm_out,
    state_ref,
    mask_ref,
    left_ref,
    right_ref,
    pbw_ref,
    pair_ref,
    outer_ref,
    wq_ref,
    wk_ref,
    wv_ref,
    wg_ref,
    wo_ref,
    up_ref,
    down_ref,
    pair_out,
    msa_out,
    load_sem,
    store_sem,
    rows,
    nf,
    ls,
    lx,
    lz,
    rz,
    tz,
    bx,
    kt,
    ka,
    sel,
    expand,
    rt,
    rt2,
    wf,
    bd,
    lhs,
    upd,
    pn,
    bi,
    bh,
    kv,
    sc,
    qs,
    gs,
    vm,
    lx_s,
    lz_s,
    lf_s,
    ka_s,
    rz_s,
    x_s,
    tz_s,
    bx_s,
    lx_r,
    lz_r,
    tz_r,
    rz_r,
    x1_r,
    bx_r,
    lf_r,
    ka_r,
    xf_r,
):
    a = lax.axis_index("aa")
    b = lax.axis_index("ba")
    core = b % 2
    chip = b // 2
    chips = n // 2
    partner = chip * 2 + 1 - core
    ns = state_ref.shape[0]
    res = state_ref.shape[1]
    ch = state_ref.shape[2]
    half = ns // 2
    opm = left_ref.shape[0]
    cz = pair_ref.shape[2]
    heads = pbw_ref.shape[0]
    wide = res * opm
    per = 128 // opm
    parts = 4
    mine = b % parts
    span = wide // parts

    first = (state_hbm, mask_hbm, left_hbm, right_hbm, pbw_hbm)
    hbm = (outer_hbm, wq_hbm, wg_hbm, pair_hbm, wk_hbm, wv_hbm, wo_hbm, up_hbm, down_hbm)
    first_to = (state_ref, mask_ref, left_ref, right_ref, pbw_ref)
    local = (outer_ref, wq_ref, wg_ref, pair_ref, wk_ref, wv_ref, wo_ref, up_ref, down_ref)
    firsts = [
        pltpu.make_async_copy(src, dst, load_sem.at[len(hbm) + k])
        for k, (src, dst) in enumerate(zip(first, first_to))
    ]
    loads = [
        pltpu.make_async_copy(src, dst, load_sem.at[k])
        for k, (src, dst) in enumerate(zip(hbm, local))
    ]

    def row_peer(t):
        c = (chip + near_to_far(t // 2) + chips) % chips
        return c * 2 + t % 2

    def col_peer(t):
        return (a + near_to_far(t) + n) % n

    for load in firsts:
        load.start()
    barrier = pltpu.get_barrier_semaphore()

    def greet(t, _):
        pl.semaphore_signal(
            barrier, inc=1, device_id={"ba": (b + t) % n}, device_id_type=pl.DeviceIdType.MESH
        )
        pl.semaphore_signal(
            barrier, inc=1, device_id={"aa": (a + t) % n}, device_id_type=pl.DeviceIdType.MESH
        )
        return 0

    lax.fori_loop(1, n, greet, 0)

    for load in loads:
        load.start()

    for load in firsts:
        load.wait()
    state = state_ref[...].reshape(ns * res, ch).astype(F32)
    normed = row_norm(state).astype(BF16)
    rows[:, b] = normed.reshape(ns, res, ch)
    for q in range(ch // 128):
        nf[q] = normed[:, q * 128 : (q + 1) * 128].astype(F32)
    by_res = jnp.concatenate(
        [
            jnp.concatenate(
                [nf[q, pl.ds(r, ns, stride=res), :] for r in range(res)], axis=0
            ).astype(BF16)
            for q in range(ch // 128)
        ],
        axis=1,
    )
    lane = lax.broadcasted_iota(jnp.int32, (opm, 128), 1)
    line = lax.broadcasted_iota(jnp.int32, (opm, 128), 0)
    rep = jnp.where(lane % opm == line, 1.0, 0.0).astype(BF16)
    lane_t = lax.broadcasted_iota(jnp.int32, (128, opm), 1)
    line_t = lax.broadcasted_iota(jnp.int32, (128, opm), 0)
    rep_t = jnp.where(line_t % opm == lane_t, 1.0, 0.0).astype(BF16)
    seg = lax.broadcasted_iota(jnp.int32, (ns, 128), 1) // opm
    keep = mask_ref[...].astype(F32).astype(BF16)
    lane_w = lax.broadcasted_iota(jnp.int32, (res, wide), 1) // opm
    line_w = lax.broadcasted_iota(jnp.int32, (res, wide), 0)
    keep_wide = mm(keep, jnp.where(lane_w == line_w, 1.0, 0.0).astype(BF16))
    keep_rep = mm(keep, rep).astype(BF16)

    def pick(parts):
        out = parts[0]
        for k in range(1, per):
            out = jnp.where(seg == k, parts[k], out)
        return out

    def factor(w_ref):
        y = mm_nt(by_res, mm(rep_t, w_ref[...]).astype(BF16))
        cols = [
            pick([y[(q * per + k) * ns : (q * per + k + 1) * ns] for k in range(per)])
            for q in range(res // per)
        ]
        return (jnp.concatenate(cols, axis=1) * keep_wide).astype(BF16)

    left = factor(left_ref)
    for k in range(parts):
        ls[k, :, :span] = left[:, k * span : (k + 1) * span]
        ls[k, :, span:] = keep_rep
    lx[b] = ls[mine]
    rz[a, :, :wide] = factor(right_ref)
    rz[a, :, wide:] = keep_rep

    pl.semaphore_wait(barrier, 2 * (n - 1))

    def to_row(buf, src, i, who, ss, rs):
        return pltpu.make_async_remote_copy(
            src_ref=src,
            dst_ref=buf,
            send_sem=ss,
            recv_sem=rs.at[i],
            device_id={"ba": who},
            device_id_type=pl.DeviceIdType.MESH,
        )

    def to_col(buf, src, i, who, ss, rs):
        return pltpu.make_async_remote_copy(
            src_ref=src,
            dst_ref=buf,
            send_sem=ss,
            recv_sem=rs.at[i],
            device_id={"aa": who},
            device_id_type=pl.DeviceIdType.MESH,
        )

    def lx_copy(i, who):
        return to_row(lx.at[i], ls.at[who % parts], i, who, lx_s, lx_r)

    def lz_copy(i, who):
        return to_col(lz.at[i, mine], lx.at[who, :, pl.ds(0, span)], i, who, lz_s, lz_r)

    def lf_copy(i, q, k, src=None):
        part = lz.at[i, q]
        return pltpu.make_async_remote_copy(
            src_ref=part if src is None else src,
            dst_ref=part,
            send_sem=lf_s,
            recv_sem=lf_r,
            device_id={"ba": b - mine + (mine + k) % parts},
            device_id_type=pl.DeviceIdType.MESH,
        )

    def ka_copy(who):
        return pltpu.make_async_remote_copy(
            src_ref=kt,
            dst_ref=ka,
            send_sem=ka_s,
            recv_sem=ka_r,
            device_id={"ba": who},
            device_id_type=pl.DeviceIdType.MESH,
        )

    def bx_copy(i, who):
        return pltpu.make_async_remote_copy(
            src_ref=tz.at[who],
            dst_ref=bx.at[i],
            send_sem=bx_s,
            recv_sem=bx_r,
            device_id={"ba": who},
            device_id_type=pl.DeviceIdType.MESH,
        )

    turn = n // 2

    def hop(buf, ss, rs, d, step, way):
        i = (a + n - way * d) % n
        part = buf.at[i]
        return pltpu.make_async_remote_copy(
            src_ref=part,
            dst_ref=part,
            send_sem=ss,
            recv_sem=rs(i, d + step, way),
            device_id={"aa": (a + n + way * step) % n},
            device_id_type=pl.DeviceIdType.MESH,
        )

    def spread(buf, ss, rs, d, reach):
        def one(step, way):
            hop(buf, ss, rs, d, step, way).start()

        for step in range(min(reach, turn - d), 0, -1):
            for way in (1, -1):
                if d + step < turn:
                    one(step, way)
                else:
                    pl.when(core == (1 - way) // 2)(functools.partial(one, step, way))

    def ring(buf, ss, rs, reach, first, last, landed):
        for d in range(first, last + 1):
            for way in (1, -1):
                if d < turn or way > 0:
                    hop(buf, ss, rs, d, 0, way).wait_recv()
            if d % reach == 0:
                spread(buf, ss, rs, d, reach)
            for way in (1, -1):
                if d < turn or way > 0:
                    landed((a + n - way * d) % n)

    def tz_at(i, d, way):
        return tz_r.at[i]

    reach = 4
    passed = [d for d in range(reach, turn, reach)]

    def rz_at(i, d, way):
        if d in passed:
            return rz_r.at[1 + 2 * passed.index(d) + (1 - way) // 2]
        return rz_r.at[0]

    def all_sent(sem, part):
        pltpu.make_async_remote_copy(
            src_ref=part,
            dst_ref=part,
            send_sem=sem,
            recv_sem=sem,
            device_id={"ba": partner},
            device_id_type=pl.DeviceIdType.MESH,
        ).wait_send()

    def all_here(sem, part):
        pltpu.make_async_remote_copy(
            src_ref=part,
            dst_ref=part,
            send_sem=sem,
            recv_sem=sem,
            device_id={"ba": partner},
            device_id_type=pl.DeviceIdType.MESH,
        ).wait_recv()

    across = chips // 2

    def x_to(i, c, step, way, d):
        part = rows.at[pl.ds(half * c, half), i]
        who = ((chip + chips + way * step) % chips) * 2 + c
        return pltpu.make_async_remote_copy(
            src_ref=part,
            dst_ref=part,
            send_sem=x_s,
            recv_sem=x1_r.at[(d + 1) // 2],
            device_id={"ba": who},
            device_id_type=pl.DeviceIdType.MESH,
        )

    def x_first():
        def one(step, way, c):
            x_to(b, c, step, way, step).start()

        for step in range(min(2, across), 0, -1):
            for way in (1, -1):
                for c in range(2):
                    if step < across:
                        one(step, way, c)
                    else:
                        pl.when(core == (1 - way) // 2)(functools.partial(one, step, way, c))

    def x_on():
        for step in range(min(2, across - 2), 0, -1):
            for way in (1, -1):
                for c in range(2):
                    if 2 + step < across or c == (1 - way) // 2:
                        i = ((chip + chips - 2 * way) % chips) * 2 + c
                        x_to(i, core, step, way, 2 + step).start()

    def x_blocks(first, last):
        return [
            ((chip + chips - way * d) % chips) * 2 + c
            for d in range(first, min(last, across) + 1)
            for way in (1, -1)
            if d < across or way > 0
            for c in range(2)
        ]

    def xf_copy(i, c, sem):
        part = rows.at[pl.ds(half * c, half), i]
        return pltpu.make_async_remote_copy(
            src_ref=part,
            dst_ref=part,
            send_sem=x_s,
            recv_sem=sem,
            device_id={"ba": partner},
            device_id_type=pl.DeviceIdType.MESH,
        )

    def start_l_off(t, _):
        lx_copy(b, row_peer(n - 1 - t)).start()
        return 0

    lx_copy(b, partner).start()
    lax.fori_loop(0, n - 2, start_l_off, 0)
    spread(rz, rz_s, rz_at, 0, reach)
    x_first()
    xf_copy(b, 1 - core, xf_r).start()
    xf_copy(b, core, xf_r).start()

    loads[0].wait()
    wf[...] = outer_ref[...].astype(F32)

    def build(d, _):
        w = wf[pl.ds(d, opm, stride=opm), :].astype(BF16)
        zero = jnp.zeros_like(w)
        for k in range(per):
            bd[pl.ds(d * 128 + k * opm, opm), :] = jnp.concatenate(
                [w if m == k else zero for m in range(per)], axis=1
            )
        return 0

    lax.fori_loop(0, opm, build, 0)

    lane_e = lax.broadcasted_iota(jnp.int32, (128, res * res), 1)
    line_e = lax.broadcasted_iota(jnp.int32, (128, res * res), 0)
    sel[...] = jnp.where(lane_e == line_e * res, 1.0, 0.0).astype(BF16)
    expand[...] = jnp.where(lane_e // res == line_e, 1.0, 0.0).astype(BF16)

    def pass_left(t, _):
        i = row_peer(t)

        @pl.when(i != b)
        def _():
            lx_copy(i, b).wait_recv()

        @pl.when(i != a)
        def _():
            lz_copy(a, i).start()

        @pl.when(i == a)
        def _():
            lz[a, mine] = lx[i, :, :span]
            for k in range(1, parts):
                lf_copy(a, mine, k, lx.at[i, :, pl.ds(0, span)]).start()

        return 0

    def nothing(i):
        pass

    lax.fori_loop(0, n * 5 // 8, pass_left, 0)
    lax.fori_loop(n * 5 // 8, n, pass_left, 0)

    for d in passed:
        for way in (1, -1):
            hop(rz, rz_s, rz_at, d, 0, way).wait_recv()
        spread(rz, rz_s, rz_at, d, reach)

    loads[1].wait()
    loads[2].wait()
    qs[...] = (mm(normed, wq_ref[...]) * ((ch // heads) ** (-0.5))).astype(BF16)
    gs[...] = jax.nn.sigmoid(mm(normed, wg_ref[...]))
    for q in range(n // per):
        vm[:, q * 128 : (q + 1) * 128] = pick(
            [lx[q * per + k, :, span:].astype(F32) for k in range(per)]
        )

    def share_left(t, _):
        i = col_peer(t)
        lz_copy(i, a).wait_recv()
        for k in range(1, parts):
            lf_copy(i, mine, k).start()
        return 0

    lax.fori_loop(1, n, share_left, 0)
    all_here(rz_r.at[0], rz.at[pl.ds(0, n - 1 - 2 * len(passed))])
    kt[...] = rz[:, :, wide:].astype(F32).reshape(n * ns, 128).T[:res].astype(BF16)

    def send_keep(t, _):
        ka_copy((b + t) % n).start()
        return 0

    @pl.when(a == b)
    def _():
        lax.fori_loop(1, n, send_keep, 0)
        ka[...] = kt[...]

    for q in range(wide // 128):
        block = rz[:, :, q * 128 : (q + 1) * 128].astype(F32).reshape(n * ns, 128)
        rt[q * 128 : (q + 1) * 128, :] = block.T

    def reorder(d, _):
        rt2[pl.ds(pl.multiple_of(d * res, res), res), :] = rt[
            pl.ds(d, res, stride=opm), :
        ].astype(BF16)
        return 0

    lax.fori_loop(0, opm, reorder, 0)


    def pass_rows(first, last, then):
        blocks = x_blocks(first, last)
        if blocks:
            many = rows.at[pl.ds(0, half), pl.ds(0, len(blocks))]
            all_here(x1_r.at[(last + 1) // 2], many)
        then()
        for i in blocks:
            xf_copy(i, core, xf_r).start()

    pass_rows(1, 2, x_on)
    def outer(k, _):
        g = (mine + k) % parts
        left = lz[:, g].astype(F32).reshape(n * ns, span).astype(BF16)
        block = mm(rt2[...], left).astype(BF16)
        for k in range(span // 128):
            at = pl.ds(pl.multiple_of((span // 128 * g + k) * res, res), res)
            for d in range(opm):
                lhs[at, d * 128 : (d + 1) * 128] = block[
                    d * res : (d + 1) * res, k * 128 : (k + 1) * 128
                ]
        return 0

    outer(0, 0)
    all_here(lf_r, lz.at[:, pl.ds(0, parts - 1)])
    lax.fori_loop(1, parts, outer, 0)
    upd[...] = mm(lhs[...], bd[...])


    @pl.when(a != b)
    def _():
        ka_copy(a).wait_recv()

    inverse = 1.0 / mm_nt(kt[...], ka[...])
    loads[3].wait()
    step = 8
    for at in range(0, res, step):
        block = jnp.concatenate(
            [
                upd[i // per * res : (i // per + 1) * res, i % per * 128 : (i % per + 1) * 128]
                * inverse[:, i : i + 1]
                for i in range(at, at + step)
            ],
            axis=0,
        )
        old = pair_ref[at : at + step].reshape(step * res, cz).astype(F32)
        fresh = (old + block).astype(BF16)
        pair_out[at : at + step] = fresh.reshape(step, res, cz)
        pn[at * res : (at + step) * res, :] = row_norm(fresh.astype(F32)).astype(BF16)
    tile = mm_nt(pbw_ref[...], pn[...])
    lane_t = lax.broadcasted_iota(jnp.int32, (heads, 128), 1)
    base = []
    for v in range(res // per):
        top = tile[:, v * 128 : (v + 1) * 128]
        by = 1
        while by < res:
            other = jnp.where(
                lane_t // by % 2 == 1, pltpu.roll(top, by, 1), pltpu.roll(top, 128 - by, 1)
            )
            top = jnp.maximum(top, other)
            by *= 2
        base.append(top)
    base = jnp.concatenate(base, axis=1).astype(BF16)
    tz[a, :, : res * res] = (tile - base.astype(F32)).astype(BF16)
    tz[a, :, res * res :] = mm_nt(base, sel[...]).astype(BF16)
    spread(tz, tz_s, tz_at, 0, 3)
    store = pltpu.make_async_copy(pair_out, pair_hbm_out, store_sem.at[0])
    store.start()

    pass_rows(3, 4, lambda: None)
    def pass_bias(i):
        @pl.when(i != b)
        def _():
            bx_copy(b, i).start()

        @pl.when(i == b)
        def _():
            bx[b] = tz[i]

    pass_bias(a)
    ring(tz, tz_s, tz_at, 3, 1, min(3, turn), pass_bias)
    all_here(xf_r, rows.at[pl.ds(0, half), pl.ds(0, n)])
    head_lane = lax.broadcasted_iota(jnp.int32, (res, ch), 1) // (ch // heads)

    loads[4].wait()
    loads[5].wait()

    def score(s, _):
        x = rows[s].reshape(n * res, ch)
        key = mm(x, wk_ref[...]).astype(BF16)
        kv[s] = mm(x, wv_ref[...]).astype(BF16)
        q = qs[pl.ds(pl.multiple_of(s * res, res), res), :].astype(F32)
        query = jnp.concatenate(
            [jnp.where(head_lane == h, q, 0.0) for h in range(heads)], axis=0
        ).astype(BF16)
        sc[s] = mm_nt(query, key)
        return 0

    lax.fori_loop(0, ns, score, 0, unroll=2)
    ring(tz, tz_s, tz_at, 3, 4, turn, pass_bias)

    others = pl.ds(0, n - 1)
    all_sent(lx_s, lx.at[others])
    all_sent(lz_s, lz.at[others, 0])
    all_sent(lf_s, lz.at[:, pl.ds(0, parts - 1)])
    all_sent(rz_s, rz.at[others])
    all_sent(x_s, rows.at[:, others])

    @pl.when(a == b)
    def _():
        all_sent(ka_s, pn.at[pl.ds(0, (n - 1) * res)])

    store.wait()
    for load in loads[6:]:
        load.wait()

    all_here(bx_r, bx.at[others])
    base = bx[:, :, res * res :].astype(F32).reshape(n * heads, 128).astype(BF16)
    base = mm(base, expand[...])
    for q in range(n // per):
        for v in range(res // per):
            cols = slice(v * 128, (v + 1) * 128)
            cut = [
                bx[q * per + k, :, cols].astype(F32)
                + base[(q * per + k) * heads : (q * per + k + 1) * heads, cols]
                for k in range(per)
            ]
            turned = [cut[0]] + [pltpu.roll(cut[k], opm * k, 1) for k in range(1, per)]
            for m in range(per):
                mixed = pick([turned[(k - m) % per] for k in range(per)])
                if m:
                    mixed = pltpu.roll(mixed, 128 - opm * m, 1)
                i = v * per + m
                bi[q, i * heads : (i + 1) * heads, :] = mixed
        for h in range(heads):
            bh[h * res : (h + 1) * res, q * 128 : (q + 1) * 128] = bi[
                q, pl.ds(h, res, stride=heads), :
            ]

    def attend(s):
        scores = jnp.where(vm[s : s + 1, :] > 0, sc[s] + bh[...], -1000000000.0)
        top = jnp.max(scores, axis=-1, keepdims=True)
        raw = jnp.exp(scores - top)
        mass = jnp.sum(raw, axis=-1, keepdims=True)
        mixed = mm(raw.astype(BF16), kv[s]) / mass
        out = mixed[:res]
        for h in range(1, heads):
            out = jnp.where(head_lane == h, mixed[h * res : (h + 1) * res], out)
        return (out * gs[s * res : (s + 1) * res, :]).astype(BF16)

    stores = []
    for k in range(2):
        these = slice(k * half, (k + 1) * half)
        gated = jnp.concatenate([attend(s) for s in range(k * half, (k + 1) * half)], axis=0)
        middle = state_ref[these].reshape(half * res, ch).astype(F32) + mm(gated, wo_ref[...])
        hidden = jnp.maximum(mm(row_norm(middle).astype(BF16), up_ref[...]), 0.0).astype(BF16)
        final = middle + mm(hidden, down_ref[...])
        msa_out[these] = final.astype(BF16).reshape(half, res, ch)
        at = pl.ds(k * half, half)
        stores.append(
            pltpu.make_async_copy(msa_out.at[at], msa_hbm_out.at[at], store_sem.at[1 + k])
        )
        stores[k].start()
    all_sent(tz_s, tz.at[others])
    all_sent(bx_s, bx.at[others])
    for store in stores:
        store.wait()


def per_device(n, *args):
    state, pair, mask, left, _, _, pbw = args[:7]
    ns, res, ch = state.shape
    opm, heads, cz = left.shape[1], pbw.shape[1], pair.shape[2]
    args = args[:3] + (left.T, args[4].T, args[5], pbw.T) + args[7:]
    wide = res * opm
    parts = 4
    span = wide // parts
    per = 128 // opm
    groups = res // per
    keys = n * res
    dma = pltpu.SemaphoreType.DMA((n,))
    vmem = pl.BlockSpec(memory_space=pltpu.VMEM)
    far = pl.BlockSpec(memory_space=pl.ANY)
    order = (0, 2, 3, 4, 6, 1, 5, 7, 8, 9, 10, 11, 12, 13)
    return tuple(
        pl.pallas_call(
            functools.partial(body, n),
            out_shape=(
                jax.ShapeDtypeStruct(state.shape, BF16),
                jax.ShapeDtypeStruct(pair.shape, BF16),
            ),
            in_specs=[far] * len(args),
            out_specs=(far, far),
            scratch_shapes=[pltpu.VMEM(args[k].shape, args[k].dtype) for k in order]
            + [
                pltpu.VMEM(pair.shape, BF16),
                pltpu.VMEM(state.shape, BF16),
                pltpu.SemaphoreType.DMA((len(order),)),
                pltpu.SemaphoreType.DMA((3,)),
                pltpu.VMEM((ns, n, res, ch), BF16),
                pltpu.VMEM((ch // 128, ns * res, 128), F32),
                pltpu.VMEM((parts, ns, span + 128), BF16),
                pltpu.VMEM((n, ns, span + 128), BF16),
                pltpu.VMEM((n, parts, ns, span), BF16),
                pltpu.VMEM((n, ns, wide + 128), BF16),
                pltpu.VMEM((n, heads, res * res + 128), BF16),
                pltpu.VMEM((n, heads, res * res + 128), BF16),
                pltpu.VMEM((res, n * ns), BF16),
                pltpu.VMEM((res, n * ns), BF16),
                pltpu.VMEM((128, res * res), BF16),
                pltpu.VMEM((128, res * res), BF16),
                pltpu.VMEM((wide, n * ns), F32),
                pltpu.VMEM((wide, n * ns), BF16),
                pltpu.VMEM((opm * opm, cz), F32),
                pltpu.VMEM((opm * 128, per * cz), BF16),
                pltpu.VMEM((groups * res, opm * 128), BF16),
                pltpu.VMEM((groups * res, per * cz), F32),
                pltpu.VMEM((res * res, cz), BF16),
                pltpu.VMEM((keys // 128, res * heads, 128), F32),
                pltpu.VMEM((heads * res, keys), F32),
                pltpu.VMEM((ns, keys, ch), BF16),
                pltpu.VMEM((ns, heads * res, keys), F32),
                pltpu.VMEM((ns * res, ch), BF16),
                pltpu.VMEM((ns * res, ch), F32),
                pltpu.VMEM((ns, keys), F32),
            ]
            + [pltpu.SemaphoreType.DMA] * 8
            + [dma] * 3
            + [pltpu.SemaphoreType.DMA((3,))] * 2
            + [pltpu.SemaphoreType.DMA] * 4,
            compiler_params=pltpu.CompilerParams(
                collective_id=0, has_side_effects=True, vmem_limit_bytes=52 * 1024 * 1024
            ),
        )(*[pltpu.with_memory_space_constraint(x, pltpu.HBM) for x in args])
    )


def solution(mesh):
    spec = P(("groups", "aa"), "ba", None)
    return jax.shard_map(
        functools.partial(per_device, mesh.shape["ba"]),
        mesh=mesh,
        in_specs=(spec, spec, P(("groups", "aa"), "ba")) + (P(),) * 11,
        out_specs=(spec, spec),
        check_vma=False,
    )
```
